256 devices in a mesh: grp: 8 (over z), row: 32 (over x, y, core).
Axes of the slice: x: 4, y: 4, z: 8, core: 2. Of those that a mesh axis runs over, the one named last changes fastest.
Arguments:
- expert_grams: float32 [4, 4096, 4096], P(None, 'row'), may hold values from -32 to 48, as said below
- expert_weights: bfloat16 [4, 4096, 1024], P(None, 'row', 'grp'), may hold values from -6 to 6
Outputs:
- merged: float32 [4096, 1024], P('row', 'grp')
- residual_ratio: float32 [], replicated
The draws below stay inside these ranges and needn't reach their ends.
Inputs may be any that keep to these rules, and one draw needn't show every extreme that they name: Each expert_grams[k] is exactly symmetric and positive definite.
All inputs are finite; a program needn't handle non-finite values.
Results may differ from the reference program's by a relative error of at most 0.0003.
Values may be sent and summed in bfloat16 or wider, within the bound.
A program may use at most 64 MiB of HBM per device.

```python
import jax
import jax.numpy as jnp
from jax import lax

D = 4096
EXPERTS = 4
ITERS = 4
COLS = 1024


def one_gram(key, expert_index):
    expert_key = jax.random.fold_in(key, 7919 + expert_index)
    sample_key, diagonal_key, common_key = jax.random.split(expert_key, 3)
    samples = D // 8
    samples_matrix = jnp.clip(jax.random.normal(sample_key, (samples, D), jnp.float32), -4.0, 4.0)
    diagonal = jnp.exp(jax.random.uniform(diagonal_key, (D,), jnp.float32, jnp.log(0.05), 0.0))
    raw_gram = jnp.dot(samples_matrix.T, samples_matrix, precision=lax.Precision.HIGHEST) / samples
    return 0.5 * (raw_gram + raw_gram.T) + jnp.diag(diagonal)


def draw_expert_grams(key, part):
    stacked = jnp.stack([one_gram(key, expert) for expert in range(EXPERTS)])
    return stacked.astype(jnp.float32)


def shard_levels(rng, shape, shards, least, high):
    factor_of = 1.0
    for axis_at, blocks in shards:
        steps = jax.random.uniform(jax.random.fold_in(jax.random.fold_in(rng, 6), axis_at), (blocks,), jnp.float32, least / len(shards), high / len(shards))
        factor_of = factor_of * jnp.repeat(jnp.exp(steps), shape[axis_at] // blocks).reshape((-1,) + (1,) * (len(shape) - 1 - axis_at))
    return factor_of


def bell_draw(own_key, extent, width, limit, cuts=(), kind=jnp.bfloat16):
    values = width * jax.random.normal(own_key, extent, jnp.float32)
    if cuts:
        values = values * shard_levels(own_key, extent, cuts, -0.22, 0.18)
    return jnp.clip(values, -limit, limit).astype(kind)


def setup_inputs(seed: int = 0) -> dict:
    seeds = jax.random.split(jax.random.key(seed), 3)
    expert_grams = draw_expert_grams(jax.random.fold_in(seeds[2], 71), 0)
    expert_weights = bell_draw(seeds[1], (EXPERTS, D, COLS), 1.0, 6.0, ((1, 32), (2, 8)))
    return dict(expert_grams=expert_grams, expert_weights=expert_weights)


def reference(expert_grams, expert_weights):
    system = lax.optimization_barrier(jnp.sum(expert_grams, axis=0)) + jnp.eye(D, dtype=jnp.float32)
    target = jnp.zeros((D, COLS), jnp.float32)
    for expert in range(EXPERTS):
        target = target + jnp.dot(expert_grams[expert], expert_weights[expert].astype(jnp.float32), precision=lax.Precision.HIGHEST, preferred_element_type=jnp.float32)
    merged = jnp.zeros((D, COLS), jnp.float32)
    residual = target
    direction = target
    norm_now = lax.optimization_barrier(jnp.sum(residual * residual, axis=0))
    initial = norm_now
    for iteration in range(ITERS):
        mapped = jnp.dot(system, direction, precision=lax.Precision.HIGHEST, preferred_element_type=jnp.float32)
        step_size = norm_now / lax.optimization_barrier(jnp.sum(direction * mapped, axis=0))
        merged = merged + step_size * direction
        residual = residual - step_size * mapped
        norm_next = lax.optimization_barrier(jnp.sum(residual * residual, axis=0))
        direction = residual + norm_next / norm_now * direction
        norm_now = norm_next
    residual_ratio = jnp.sqrt(jnp.sum(norm_now) / jnp.sum(initial))
    return (merged, residual_ratio)
```

```python
import jax
import jax.numpy as jnp
from jax import lax
from jax.experimental import pallas as pl
from jax.experimental.pallas import tpu as pltpu
from jax.sharding import PartitionSpec as P

MESH = pl.DeviceIdType.MESH
F32, BF16 = jnp.float32, jnp.bfloat16
EXPERTS, ROWS, COLS = 4, 128, 128
CHIPS, SIDE, WIDE, MINE, HALF = 16, 4, 256, 64, 32


def split(x):
    high = x.astype(BF16)
    return high, (x - high.astype(F32)).astype(BF16)


def column_sum(x):
    return jnp.sum(x, axis=1, keepdims=True)


def kernel(
    grams, weights, merged, ratio,
    panel, matrix, weights_t, partial, partner_part, first, second, outgoing,
    gather_b, gather_0, gather_1, gather_2, residual, mapped_dir,
    sums, totals, answer,
    panel_sem, partner_sem, matrix_sem, first_sem, second_sem, gather_sem, sums_sem, totals_sem, answer_sem, send_sem,
):
    grp, row = lax.axis_index("grp"), lax.axis_index("row")
    core, chip = lax.rem(row, 2), lax.div(row, 2)
    x, y = lax.div(chip, SIDE), lax.rem(chip, SIDE)
    other = 1 - core

    def at(cx, cy):
        return lax.rem(cx, SIDE) * SIDE + lax.rem(cy, SIDE)

    def device(target):
        return (grp, target * 2 + core)

    partner = (grp, chip * 2 + other)

    def push(src, dst, sent, arrived, to):
        pltpu.make_async_remote_copy(src, dst, sent, arrived, device_id=to, device_id_type=MESH).start()

    def await_bytes(ref, sem):
        pltpu.make_async_copy(ref, ref, sem).wait()

    def order(n):
        return lax.rem(chip + 1 + n, CHIPS)

    def panel_copy(n):
        columns = pl.ds(pl.multiple_of(order(n) * WIDE, WIDE), WIDE)
        return pltpu.make_async_copy(grams.at[:, :, columns], panel.at[n], panel_sem.at[n])

    def fetch(n, _):
        panel_copy(n).start()
        return 0

    lax.fori_loop(0, CHIPS, fetch, 0)

    barrier = pltpu.get_barrier_semaphore()

    def greet_chip(n, _):
        pl.semaphore_signal(barrier, 1, device_id=device(lax.rem(chip + n, CHIPS)), device_id_type=MESH)
        return 0

    lax.fori_loop(1, CHIPS, greet_chip, 0)
    groups = lax.axis_size("grp")

    def greet_group(n, _):
        there = lax.rem(grp * 2 + core + n, 2 * groups)
        pl.semaphore_signal(
            barrier, 1, device_id=(lax.div(there, 2), chip * 2 + lax.rem(there, 2)), device_id_type=MESH
        )
        return 0

    lax.fori_loop(1, 2 * groups, greet_group, 0)

    stacked = weights[...].reshape(EXPERTS * ROWS, COLS).astype(F32)
    weights_t[...] = jnp.transpose(stacked).astype(BF16)
    pl.semaphore_wait(barrier, CHIPS - 1 + 2 * groups - 1)

    def compute_panel(n):
        target = order(n)
        panel_copy(n).wait()
        block = panel[n].reshape(EXPERTS * ROWS, WIDE)
        high, low = split(block)
        product = jnp.dot(weights_t[...], high, preferred_element_type=F32) + jnp.dot(
            weights_t[...], low, preferred_element_type=F32
        )
        partial[target] = product.reshape(2, MINE, WIDE)
        push(partial.at[target, other], partner_part.at[target], send_sem.at[0], partner_sem.at[target], partner)
        system = (panel[n, 0] + panel[n, 1]) + (panel[n, 2] + panel[n, 3])
        rows = lax.broadcasted_iota(jnp.int32, (ROWS, WIDE), 0) + (chip * WIDE + core * ROWS)
        columns = lax.broadcasted_iota(jnp.int32, (ROWS, WIDE), 1) + target * WIDE
        system = system + (rows == columns).astype(F32)
        system_high, system_low = split(system)
        matrix[target, core, 0] = system_high
        matrix[target, core, 1] = system_low
        push(matrix.at[target, core], matrix.at[target, core], send_sem.at[1], matrix_sem.at[target], partner)

    def forward_panel(n):
        target = order(n)
        tx, ty = lax.div(target, SIDE), lax.rem(target, SIDE)
        await_bytes(partner_part.at[target], partner_sem.at[target])
        outgoing[target] = partial[target, core] + partner_part[target]

        @pl.when(tx != x)
        def _():
            push(
                outgoing.at[target, pl.ds(0, HALF)], first.at[0, x, ty],
                send_sem.at[2], first_sem.at[0, x, ty], device(at(tx, y)),
            )

        @pl.when(ty != y)
        def _():
            push(
                outgoing.at[target, pl.ds(HALF, HALF)], first.at[1, y, tx],
                send_sem.at[2], first_sem.at[1, y, tx], device(at(x, ty)),
            )

    lag = 2

    def panel_step(n, _):
        @pl.when(n < CHIPS)
        def _():
            compute_panel(n)

        @pl.when(n >= lag)
        def _():
            forward_panel(n - lag)

        return 0

    lax.fori_loop(0, CHIPS + lag, panel_step, 0)

    def first_sum(half, k):
        line, along = (x, y) if half == 0 else (y, x)
        place = lax.rem(along + k, SIDE)
        target = at(x, place) if half == 0 else at(place, y)
        total = outgoing[target, pl.ds(half * HALF, HALF)]
        for j in (1, 3, 2):
            source = lax.rem(line + j, SIDE)
            await_bytes(first.at[half, source, place], first_sem.at[half, source, place])
            total = total + first[half, source, place]
        return total, target

    for k in (1, 3, 2):
        for half in (0, 1):
            along = y if half == 0 else x
            total, target = first_sum(half, k)
            second[half, 0, k] = total
            push(
                second.at[half, 0, k], second.at[half, 1, along],
                send_sem.at[3], second_sem.at[half, along], device(target),
            )
    pieces = []
    for half in (0, 1):
        along = y if half == 0 else x
        total, _ = first_sum(half, 0)
        for j in (1, 3, 2):
            source = lax.rem(along + j, SIDE)
            await_bytes(second.at[half, 1, source], second_sem.at[half, source])
            total = total + second[half, 1, source]
        pieces.append(total)
    own_r = jnp.concatenate(pieces, axis=0)

    def gather(index, buffer, value):
        if index < 3:
            high, low = split(value)
            for half in (0, 1):
                buffer[chip, half, 0] = high[half * HALF : (half + 1) * HALF]
                buffer[chip, half, 1] = low[half * HALF : (half + 1) * HALF]
        else:
            high = value.astype(BF16)
            for half in (0, 1):
                buffer[chip, half] = high[half * HALF : (half + 1) * HALF]

        def send(origin, half, target):
            block = buffer.at[origin, half]
            push(block, block, send_sem.at[4 + index], gather_sem.at[index, origin, half], device(target))

        def arrive(origin, half):
            await_bytes(buffer.at[origin, half], gather_sem.at[index, origin, half])

        steps = (1, 3, 2)
        for d in steps:
            send(chip, 0, at(x + d, y))
            send(chip, 1, at(x, y + d))
        for d in steps:
            send(chip, 0, at(x, y + d))
            send(chip, 1, at(x + d, y))
        for d in (3, 1, 2):
            origin = at(x + d, y)
            arrive(origin, 0)
            for e in steps:
                send(origin, 0, at(x, y + e))
            origin = at(x, y + d)
            arrive(origin, 1)
            for e in steps:
                send(origin, 1, at(x + e, y))

        def finish():
            for d in (0, 1, 3, 2):
                for e in (1, 3, 2):
                    arrive(at(x + d, y + e), 0)
                    arrive(at(x + e, y + d), 1)

        return finish

    def multiply(buffer, planes):
        height = planes * MINE
        total = None
        for q in range(SIDE):
            left = jnp.concatenate([buffer[SIDE * q + i].reshape(height, WIDE) for i in range(SIDE)], axis=1)
            right = jnp.concatenate([matrix[SIDE * q + i].reshape(2 * WIDE, WIDE) for i in range(SIDE)], axis=1)
            piece = lax.dot_general(left, right, (((1,), (1,)), ((), ())), preferred_element_type=F32)
            total = piece if total is None else total + piece
        if planes == 2:
            total = total.reshape(2, 2, HALF, 2 * WIDE)
            total = (total[:, 0] + total[:, 1]).reshape(MINE, 2 * WIDE)
        return jnp.concatenate(
            [total[:, i * WIDE : i * WIDE + ROWS] + total[:, i * WIDE + ROWS : (i + 1) * WIDE] for i in (0, 1)],
            axis=1,
        )

    def whole(buffer, planes, origin):
        if planes == 2:
            block = buffer[origin].astype(F32)
            return (block[:, 0] + block[:, 1]).reshape(MINE, WIDE)
        return buffer[origin].astype(F32).reshape(MINE, WIDE)

    zero = jnp.zeros((MINE, WIDE), F32)

    gather(0, gather_b, own_r)()
    for origin in range(CHIPS):
        await_bytes(matrix.at[origin, other], matrix_sem.at[origin])

    def load_target(origin, total):
        block = whole(gather_b, 2, origin)
        residual[origin] = block
        return total + block * block

    norm = column_sum(lax.fori_loop(0, CHIPS, load_target, zero))
    initial = norm
    own_w = multiply(gather_b, 2)

    alpha = beta = None
    own_p = own_s = own_t = own_x = None
    for step, (buffer, planes) in enumerate(((gather_0, 2), (gather_1, 2), (gather_2, 1))):
        gather(step + 1, buffer, own_w)()

        def inner(origin, total, buffer=buffer, planes=planes):
            return total + residual[origin] * whole(buffer, planes, origin)

        product = column_sum(lax.fori_loop(0, CHIPS, inner, zero))
        own_u = multiply(buffer, planes)
        if step == 0:
            alpha = norm / product
            own_p, own_s, own_t = own_r, own_w, own_u
            own_x = alpha * own_p
        else:
            alpha = norm / (product - beta * norm / alpha)
            own_p = own_r + beta * own_p
            own_s = own_w + beta * own_s
            own_t = own_u + beta * own_t
            own_x = own_x + alpha * own_p
        own_r = own_r - alpha * own_s
        own_w = own_w - alpha * own_t

        def advance(origin, total, buffer=buffer, planes=planes, step=step, alpha=alpha, beta=beta):
            direction = whole(buffer, planes, origin)
            if step > 0:
                direction = direction + beta * mapped_dir[origin]
            mapped_dir[origin] = direction
            block = residual[origin] - alpha * direction
            residual[origin] = block
            return total + block * block

        following = column_sum(lax.fori_loop(0, CHIPS, advance, zero))
        beta = following / norm
        norm = following

    own_s = own_w + beta * own_s
    own_p = own_r + beta * own_p
    near = own_r - alpha * own_s
    lane = lax.broadcasted_iota(jnp.int32, (MINE, ROWS), 1)
    packed = jnp.zeros((MINE, ROWS), F32)
    for i, terms in enumerate((own_r * own_w, near * near, near * own_s, own_s * own_s)):
        packed = jnp.where(lane == i, column_sum(terms), packed)
    packed = jnp.transpose(jnp.concatenate([packed, jnp.zeros_like(packed)], axis=0))
    sums[chip] = packed[:8]

    def tell_chip(n, _):
        push(sums.at[chip], sums.at[chip], send_sem.at[8], sums_sem.at[chip], device(lax.rem(chip + n, CHIPS)))
        return 0

    lax.fori_loop(1, CHIPS, tell_chip, 0)

    def hear_chip(n, _):
        source = lax.rem(chip + n, CHIPS)
        await_bytes(sums.at[source], sums_sem.at[source])
        return 0

    lax.fori_loop(1, CHIPS, hear_chip, 0)
    gathered = jnp.sum(sums[...], axis=0)
    gathered = jnp.transpose(jnp.concatenate([gathered, jnp.zeros((ROWS - 8, ROWS), F32)], axis=0))[:MINE]
    product, near_near, near_s, s_s = (gathered[:, i : i + 1] for i in range(4))
    last = norm / (product - beta * norm / alpha)
    own_x = own_x + last * own_p
    excess = last - alpha
    final = jnp.maximum(near_near - 2.0 * excess * near_s + excess * excess * s_s, 0.0)

    place = grp * 2 + core
    lane = lax.broadcasted_iota(jnp.int32, (MINE, ROWS), 1)
    both = jnp.where(lane == 0, final, jnp.where(lane == 1, initial, 0.0))
    totals[place] = jnp.sum(both, axis=0, keepdims=True)
    answer[core, 0] = own_x[:, :ROWS]
    answer[core, 1] = own_x[:, ROWS:]
    push(answer.at[core, other], answer.at[core, other], send_sem.at[9], answer_sem, partner)

    def tell_group(n, _):
        there = lax.rem(place + n, 2 * groups)
        push(
            totals.at[place], totals.at[place], send_sem.at[10], totals_sem.at[place],
            (lax.div(there, 2), chip * 2 + lax.rem(there, 2)),
        )
        return 0

    lax.fori_loop(1, 2 * groups, tell_group, 0)
    await_bytes(answer.at[other, core], answer_sem)
    columns = jnp.concatenate([answer[0, core], answer[1, core]], axis=0)
    merged[...] = jnp.transpose(columns)

    def hear_group(n, _):
        source = lax.rem(place + n, 2 * groups)
        await_bytes(totals.at[source], totals_sem.at[source])
        return 0

    lax.fori_loop(1, 2 * groups, hear_group, 0)
    over_all = jnp.sum(totals[...], axis=0)
    ratio[...] = jnp.sqrt(over_all[:, 0:1] / over_all[:, 1:2]) + jnp.zeros((1, ROWS), F32)

    await_bytes(partner_part, send_sem.at[0])
    await_bytes(matrix.at[:, 0], send_sem.at[1])
    await_bytes(first.at[:, pl.ds(0, 3)], send_sem.at[2])
    await_bytes(second.at[:, 0, pl.ds(0, 3)], send_sem.at[3])
    for i, buffer in enumerate((gather_b, gather_0, gather_1, gather_2)):
        await_bytes(buffer.at[pl.ds(0, CHIPS - 1)], send_sem.at[4 + i])
    await_bytes(sums.at[pl.ds(0, CHIPS - 1)], send_sem.at[8])
    await_bytes(answer.at[0, 0], send_sem.at[9])
    await_bytes(totals.at[pl.ds(0, 2 * groups - 1)], send_sem.at[10])


def local(expert_grams, expert_weights):
    groups = lax.axis_size("grp")
    vmem = pl.BlockSpec(memory_space=pltpu.VMEM)
    dma = pltpu.SemaphoreType.DMA
    merged, ratio = pl.pallas_call(
        kernel,
        out_shape=(jax.ShapeDtypeStruct((ROWS, COLS), F32), jax.ShapeDtypeStruct((1, ROWS), F32)),
        in_specs=[pl.BlockSpec(memory_space=pl.ANY), vmem],
        out_specs=(vmem, vmem),
        scratch_shapes=[
            pltpu.VMEM((CHIPS, EXPERTS, ROWS, WIDE), F32),
            pltpu.VMEM((CHIPS, 2, 2, ROWS, WIDE), BF16),
            pltpu.VMEM((COLS, EXPERTS * ROWS), BF16),
            pltpu.VMEM((CHIPS, 2, MINE, WIDE), F32),
            pltpu.VMEM((CHIPS, MINE, WIDE), F32),
            pltpu.VMEM((2, SIDE, SIDE, HALF, WIDE), F32),
            pltpu.VMEM((2, 2, SIDE, HALF, WIDE), F32),
            pltpu.VMEM((CHIPS, MINE, WIDE), F32),
            pltpu.VMEM((CHIPS, 2, 2, HALF, WIDE), BF16),
            pltpu.VMEM((CHIPS, 2, 2, HALF, WIDE), BF16),
            pltpu.VMEM((CHIPS, 2, 2, HALF, WIDE), BF16),
            pltpu.VMEM((CHIPS, 2, HALF, WIDE), BF16),
            pltpu.VMEM((CHIPS, MINE, WIDE), F32),
            pltpu.VMEM((CHIPS, MINE, WIDE), F32),
            pltpu.VMEM((CHIPS, 8, ROWS), F32),
            pltpu.VMEM((2 * groups, 1, ROWS), F32),
            pltpu.VMEM((2, 2, MINE, ROWS), F32),
            dma((CHIPS,)),
            dma((CHIPS,)),
            dma((CHIPS,)),
            dma((2, SIDE, SIDE)),
            dma((2, SIDE)),
            dma((4, CHIPS, 2)),
            dma((CHIPS,)),
            dma((2 * groups,)),
            dma,
            dma((11,)),
        ],
        compiler_params=pltpu.CompilerParams(
            collective_id=0, has_side_effects=True, vmem_limit_bytes=56 * 1024 * 1024
        ),
        name="merge",
    )(expert_grams, expert_weights)
    return merged, ratio[0, 0]


def solution(mesh):
    placed = (P(None, "row", None), P(None, "row", "grp"))
    return jax.shard_map(
        local, mesh=mesh, in_specs=placed, out_specs=(P("row", "grp"), P()), check_vma=False
    )
```

```python
import jax
import jax.numpy as jnp
from jax import lax
from jax.experimental import pallas as pl
from jax.experimental.pallas import tpu as pltpu
from jax.sharding import PartitionSpec as P

MESH = pl.DeviceIdType.MESH
F32, BF16 = jnp.float32, jnp.bfloat16
EXPERTS, ROWS, COLS = 4, 128, 128
CHIPS, SIDE, WIDE, MINE, HALF = 16, 4, 256, 64, 32


def split(x):
    high = x.astype(BF16)
    return high, (x - high.astype(F32)).astype(BF16)


def column_sum(x):
    return jnp.sum(x, axis=1, keepdims=True)


def kernel(
    grams, weights, merged, ratio,
    panel, matrix, weights_in, weights_t, partial, partner_part, first, second, outgoing,
    gather_b, gather_0, gather_1, gather_2, residual, mapped_dir, dots, product,
    sums, totals, answer, merged_out, ratio_out,
    panel_sem, partner_sem, matrix_sem, first_sem, second_sem, gather_sem, sums_sem, totals_sem, answer_sem,
    send_sem, local_sem,
):
    grp, row = lax.axis_index("grp"), lax.axis_index("row")
    core, chip = lax.rem(row, 2), lax.div(row, 2)
    x, y = lax.div(chip, SIDE), lax.rem(chip, SIDE)
    other = 1 - core

    def at(cx, cy):
        return lax.rem(cx, SIDE) * SIDE + lax.rem(cy, SIDE)

    def device(target):
        return (grp, target * 2 + core)

    partner = (grp, chip * 2 + other)

    def push(src, dst, sent, arrived, to):
        pltpu.make_async_remote_copy(src, dst, sent, arrived, device_id=to, device_id_type=MESH).start()

    def await_bytes(ref, sem):
        pltpu.make_async_copy(ref, ref, sem).wait()

    weights_copy = pltpu.make_async_copy(weights, weights_in, local_sem.at[0])
    weights_copy.start()

    def panel_copy(n):
        columns = pl.ds(pl.multiple_of(n * WIDE, WIDE), WIDE)
        return pltpu.make_async_copy(grams.at[:, :, columns], panel.at[n], panel_sem.at[n])

    def fetch(n, _):
        panel_copy(n).start()
        return 0

    lax.fori_loop(0, CHIPS, fetch, 0)

    barrier = pltpu.get_barrier_semaphore()

    def greet_chip(n, _):
        pl.semaphore_signal(barrier, 1, device_id=device(lax.rem(chip + n, CHIPS)), device_id_type=MESH)
        return 0

    lax.fori_loop(1, CHIPS, greet_chip, 0)
    groups = lax.axis_size("grp")

    def greet_group(n, _):
        there = lax.rem(grp * 2 + core + n, 2 * groups)
        pl.semaphore_signal(
            barrier, 1, device_id=(lax.div(there, 2), chip * 2 + lax.rem(there, 2)), device_id_type=MESH
        )
        return 0

    lax.fori_loop(1, 2 * groups, greet_group, 0)

    weights_copy.wait()
    turned = jnp.transpose(weights_in[...].reshape(EXPERTS * ROWS, COLS).astype(F32)).astype(BF16)
    weights_t[:, : EXPERTS * ROWS] = turned
    weights_t[:, EXPERTS * ROWS :] = turned

    def compute_panel(target):
        panel_copy(target).wait()
        high, low = split(panel[target].reshape(EXPERTS * ROWS, WIDE))
        product = jnp.dot(weights_t[...], jnp.concatenate([high, low], axis=0), preferred_element_type=F32)
        partial[target] = product.reshape(2, MINE, WIDE)
        system = (panel[target, 0] + panel[target, 1]) + (panel[target, 2] + panel[target, 3])
        rows = lax.broadcasted_iota(jnp.int32, (ROWS, WIDE), 0) + (chip * WIDE + core * ROWS)
        columns = lax.broadcasted_iota(jnp.int32, (ROWS, WIDE), 1) + target * WIDE
        system_high, system_low = split(system + (rows == columns).astype(F32))
        matrix[target, core, 0] = system_high
        matrix[target, core, 1] = system_low

    def panel_step(n, _):
        for i in range(4):
            compute_panel(4 * n + i)
        return 0

    lax.fori_loop(0, CHIPS // 4, panel_step, 0)

    pl.semaphore_wait(barrier, CHIPS - 1 + 2 * groups - 1)

    targets = [(2, 2), (1, 2), (3, 2), (2, 1), (2, 3), (1, 1), (3, 1), (1, 3), (3, 3)]
    targets += [(0, 2), (2, 0), (0, 1), (1, 0), (0, 3), (3, 0), (0, 0)]
    for dx, dy in targets:
        target = at(x + dx, y + dy)
        push(partial.at[target, other], partner_part.at[target], send_sem.at[0], partner_sem.at[target], partner)
    for dx, dy in targets:
        target = at(x + dx, y + dy)
        await_bytes(partner_part.at[target], partner_sem.at[target])
        outgoing[target] = partial[target, core] + partner_part[target]
        if dx != 0:
            push(
                outgoing.at[target, pl.ds(0, HALF)], first.at[0, x, lax.rem(y + dy, SIDE)],
                send_sem.at[2], first_sem.at[0, x, lax.rem(y + dy, SIDE)], device(at(x + dx, y)),
            )
        if dy != 0:
            push(
                outgoing.at[target, pl.ds(HALF, HALF)], first.at[1, y, lax.rem(x + dx, SIDE)],
                send_sem.at[2], first_sem.at[1, y, lax.rem(x + dx, SIDE)], device(at(x, y + dy)),
            )

    def first_sum(half, k):
        line, along = (x, y) if half == 0 else (y, x)
        place = lax.rem(along + k, SIDE)
        target = at(x, place) if half == 0 else at(place, y)
        total = outgoing[target, pl.ds(half * HALF, HALF)]
        for j in (1, 3, 2):
            source = lax.rem(line + j, SIDE)
            await_bytes(first.at[half, source, place], first_sem.at[half, source, place])
            total = total + first[half, source, place]
        return total, target

    for k in (2, 1, 3):
        for half in (0, 1):
            along = y if half == 0 else x
            total, target = first_sum(half, k)
            second[half, 0, k] = total
            push(
                second.at[half, 0, k], second.at[half, 1, along],
                send_sem.at[3], second_sem.at[half, along], device(target),
            )
    def send_matrix(target, _):
        push(matrix.at[target, core], matrix.at[target, core], send_sem.at[1], matrix_sem, partner)
        return 0

    lax.fori_loop(0, CHIPS, send_matrix, 0)

    pieces = []
    for half in (0, 1):
        along = y if half == 0 else x
        total, _ = first_sum(half, 0)
        for j in (1, 3, 2):
            source = lax.rem(along + j, SIDE)
            await_bytes(second.at[half, 1, source], second_sem.at[half, source])
            total = total + second[half, 1, source]
        pieces.append(total)
    own_r = jnp.concatenate(pieces, axis=0)

    near_blocks = [(0, 0), (1, 0), (3, 0), (0, 1), (0, 3), (2, 0), (0, 2)]
    middle_blocks = [(1, 1), (1, 3), (3, 1), (3, 3)]
    far_blocks = [(2, 1), (2, 3), (1, 2), (3, 2), (2, 2)]

    def place_of(dx, dy, half):
        if dx != 0 and dy != 0:
            return 0 if 2 in (dx, dy) else 8
        if half == 0:
            return dx if dy == 0 else 7
        return 3 + dy if dx == 0 else 7

    class Gather:
        def __init__(self, index, buffer):
            self.index, self.buffer = index, buffer

        def send(self, dx, dy, half, ex, ey):
            block = self.buffer.at[at(x + dx, y + dy), half]
            place = place_of((dx - ex) % SIDE, (dy - ey) % SIDE, half)
            push(block, block, send_sem.at[4 + self.index], gather_sem.at[self.index, place], device(at(x + ex, y + ey)))

        def arrive(self, place, ref):
            await_bytes(ref, gather_sem.at[self.index, place])

        def start(self, value):
            buffer = self.buffer
            high, low = split(value)
            for half in (0, 1):
                here = slice(half * HALF, (half + 1) * HALF)
                if self.index < 3:
                    buffer[chip, half, 0] = high[here]
                    buffer[chip, half, 1] = low[here]
                else:
                    buffer[chip, half] = high[here]
            for d in (1, 3, 2):
                self.send(0, 0, 0, d, 0)
                self.send(0, 0, 1, 0, d)
            for d in (2, 1, 3):
                self.send(0, 0, 0, 0, d)
                self.send(0, 0, 1, d, 0)

        def forward(self):
            half_block = self.buffer.at[0, 0]
            for d in (1, 3, 2):
                self.arrive(d, half_block)
                for e in (2, 1, 3):
                    self.send(d, 0, 0, 0, e)
                self.arrive(3 + d, half_block)
                for e in (2, 1, 3):
                    self.send(0, d, 1, e, 0)

        def near(self):
            self.arrive(7, self.buffer.at[pl.ds(0, 3)])

        def middle(self):
            self.arrive(8, self.buffer.at[pl.ds(0, 4)])

        def far(self):
            self.arrive(0, self.buffer.at[pl.ds(0, 5)])

    def multiply(buffer, planes, blocks):
        places = [at(x + dx, y + dy) for dx, dy in blocks]
        left = jnp.concatenate([buffer[i].reshape(planes * MINE, WIDE) for i in places], axis=1)
        right = jnp.concatenate([matrix[i].reshape(2 * WIDE, WIDE) for i in places], axis=1)
        return lax.dot_general(left, right, (((1,), (1,)), ((), ())), preferred_element_type=F32)

    def fold(total, planes):
        if planes == 2:
            total = total.reshape(2, 2, HALF, 2 * WIDE)
            total = (total[:, 0] + total[:, 1]).reshape(MINE, 2 * WIDE)
        return jnp.concatenate(
            [total[:, i * WIDE : i * WIDE + ROWS] + total[:, i * WIDE + ROWS : (i + 1) * WIDE] for i in (0, 1)],
            axis=1,
        )

    def whole(buffer, planes, origin):
        block = buffer[origin].astype(F32)
        if planes == 2:
            block = block[:, 0] + block[:, 1]
        return block.reshape(MINE, WIDE)

    def products(gather, planes, blocks, first_time):
        for dx, dy in blocks:
            origin = at(x + dx, y + dy)
            block = whole(gather.buffer, planes, origin)
            if first_time:
                residual[origin] = block
                terms = block * block
            else:
                terms = residual[origin] * block
            dots[origin] = terms[:, :ROWS] + terms[:, ROWS:]
        return multiply(gather.buffer, planes, blocks)

    def finish(gather, planes, first_time=False):
        gather.forward()
        gather.near()
        height = planes * MINE
        product[:height] = products(gather, planes, near_blocks, first_time)
        gather.middle()
        product[:height] = product[:height] + products(gather, planes, middle_blocks, first_time)
        gather.far()
        total = product[:height] + products(gather, planes, far_blocks, first_time)
        return fold(total, planes), column_sum(jnp.sum(dots[...], axis=0))

    zero = jnp.zeros((MINE, WIDE), F32)

    gather = Gather(0, gather_b)
    gather.start(own_r)
    await_bytes(matrix.at[:, other], matrix_sem)
    own_w, norm = finish(gather, 2, True)
    initial = norm

    alpha = beta = None
    own_p = own_s = own_t = own_x = None
    for step, (buffer, planes) in enumerate(((gather_0, 2), (gather_1, 2), (gather_2, 1))):
        gather = Gather(step + 1, buffer)
        gather.start(own_w)
        if step > 0:
            before, before_planes = ((gather_0, 2), (gather_1, 2))[step - 1]

            def advance(origin, total, buffer=before, planes=before_planes, step=step, alpha=alpha, beta=old_beta):
                direction = whole(buffer, planes, origin)
                if step > 1:
                    direction = direction + beta * mapped_dir[origin]
                mapped_dir[origin] = direction
                block = residual[origin] - alpha * direction
                residual[origin] = block
                return total + block * block

            following = column_sum(lax.fori_loop(0, CHIPS, advance, zero))
            beta = following / norm
            norm = following
        own_u, overlap = finish(gather, planes)
        if step == 0:
            alpha = norm / overlap
            own_p, own_s, own_t = own_r, own_w, own_u
            own_x = alpha * own_p
        else:
            alpha = norm / (overlap - beta * norm / alpha)
            own_p = own_r + beta * own_p
            own_s = own_w + beta * own_s
            own_t = own_u + beta * own_t
            own_x = own_x + alpha * own_p
        old_beta = beta
        own_r = own_r - alpha * own_s
        own_w = own_w - alpha * own_t

    def last_advance(origin, total):
        direction = whole(gather_2, 1, origin) + beta * mapped_dir[origin]
        block = residual[origin] - alpha * direction
        return total + block * block

    following = column_sum(lax.fori_loop(0, CHIPS, last_advance, zero))
    beta = following / norm
    norm = following

    own_s = own_w + beta * own_s
    own_p = own_r + beta * own_p
    close = own_r - alpha * own_s
    lane = lax.broadcasted_iota(jnp.int32, (MINE, ROWS), 1)
    packed = jnp.zeros((MINE, ROWS), F32)
    for i, terms in enumerate((own_r * own_w, close * close, close * own_s, own_s * own_s)):
        packed = jnp.where(lane == i, column_sum(terms), packed)
    packed = jnp.transpose(jnp.concatenate([packed, jnp.zeros_like(packed)], axis=0))
    sums[chip] = packed[:8]

    def tell_chip(n, _):
        push(sums.at[chip], sums.at[chip], send_sem.at[8], sums_sem, device(lax.rem(chip + n, CHIPS)))
        return 0

    lax.fori_loop(1, CHIPS, tell_chip, 0)
    await_bytes(sums.at[pl.ds(0, CHIPS - 1)], sums_sem)
    gathered = jnp.sum(sums[...], axis=0)
    gathered = jnp.transpose(jnp.concatenate([gathered, jnp.zeros((ROWS - 8, ROWS), F32)], axis=0))[:MINE]
    overlap, close_close, close_s, s_s = (gathered[:, i : i + 1] for i in range(4))
    last = norm / (overlap - beta * norm / alpha)
    excess = last - alpha
    final = jnp.maximum(close_close - 2.0 * excess * close_s + excess * excess * s_s, 0.0)

    place = grp * 2 + core
    both = jnp.where(lane == 0, final, jnp.where(lane == 1, initial, 0.0))
    totals[place] = jnp.sum(both, axis=0, keepdims=True)

    def tell_group(n, _):
        there = lax.rem(place + n, 2 * groups)
        push(
            totals.at[place], totals.at[place], send_sem.at[10], totals_sem,
            (lax.div(there, 2), chip * 2 + lax.rem(there, 2)),
        )
        return 0

    lax.fori_loop(1, 2 * groups, tell_group, 0)
    own_x = own_x + last * own_p
    answer[core, 0] = own_x[:, :ROWS]
    answer[core, 1] = own_x[:, ROWS:]
    push(answer.at[core, other], answer.at[core, other], send_sem.at[9], answer_sem, partner)
    await_bytes(answer.at[other, core], answer_sem)
    merged_out[...] = jnp.transpose(jnp.concatenate([answer[0, core], answer[1, core]], axis=0))
    merged_copy = pltpu.make_async_copy(merged_out, merged, local_sem.at[1])
    merged_copy.start()

    await_bytes(partner_part, send_sem.at[0])
    await_bytes(matrix.at[:, 0], send_sem.at[1])
    await_bytes(first.at[:, pl.ds(0, 3)], send_sem.at[2])
    await_bytes(second.at[:, 0, pl.ds(0, 3)], send_sem.at[3])
    for i, buffer in enumerate((gather_b, gather_0, gather_1, gather_2)):
        await_bytes(buffer.at[pl.ds(0, CHIPS - 1)], send_sem.at[4 + i])
    await_bytes(sums.at[pl.ds(0, CHIPS - 1)], send_sem.at[8])
    await_bytes(answer.at[0, 0], send_sem.at[9])
    await_bytes(totals.at[pl.ds(0, 2 * groups - 1)], send_sem.at[10])
    merged_copy.wait()
    await_bytes(totals.at[pl.ds(0, 2 * groups - 1)], totals_sem)
    over_all = jnp.sum(totals[...], axis=0)
    ratio_out[...] = jnp.sqrt(over_all[:, 0:1] / over_all[:, 1:2]) + jnp.zeros((1, ROWS), F32)
    ratio_copy = pltpu.make_async_copy(ratio_out, ratio, local_sem.at[0])
    ratio_copy.start()
    ratio_copy.wait()


def local(expert_grams, expert_weights):
    groups = lax.axis_size("grp")
    hbm = pl.BlockSpec(memory_space=pltpu.HBM)
    anywhere = pl.BlockSpec(memory_space=pl.ANY)
    dma = pltpu.SemaphoreType.DMA
    merged, ratio = pl.pallas_call(
        kernel,
        out_shape=(jax.ShapeDtypeStruct((ROWS, COLS), F32), jax.ShapeDtypeStruct((1, ROWS), F32)),
        in_specs=[hbm, hbm],
        out_specs=(anywhere, anywhere),
        scratch_shapes=[
            pltpu.VMEM((CHIPS, EXPERTS, ROWS, WIDE), F32),
            pltpu.VMEM((CHIPS, 2, 2, ROWS, WIDE), BF16),
            pltpu.VMEM((EXPERTS, ROWS, COLS), BF16),
            pltpu.VMEM((COLS, 2 * EXPERTS * ROWS), BF16),
            pltpu.VMEM((CHIPS, 2, MINE, WIDE), F32),
            pltpu.VMEM((CHIPS, MINE, WIDE), F32),
            pltpu.VMEM((2, SIDE, SIDE, HALF, WIDE), F32),
            pltpu.VMEM((2, 2, SIDE, HALF, WIDE), F32),
            pltpu.VMEM((CHIPS, MINE, WIDE), F32),
            pltpu.VMEM((CHIPS, 2, 2, HALF, WIDE), BF16),
            pltpu.VMEM((CHIPS, 2, 2, HALF, WIDE), BF16),
            pltpu.VMEM((CHIPS, 2, 2, HALF, WIDE), BF16),
            pltpu.VMEM((CHIPS, 2, HALF, WIDE), BF16),
            pltpu.VMEM((CHIPS, MINE, WIDE), F32),
            pltpu.VMEM((CHIPS, MINE, WIDE), F32),
            pltpu.VMEM((CHIPS, MINE, ROWS), F32),
            pltpu.VMEM((2 * MINE, 2 * WIDE), F32),
            pltpu.VMEM((CHIPS, 8, ROWS), F32),
            pltpu.VMEM((2 * groups, 1, ROWS), F32),
            pltpu.VMEM((2, 2, MINE, ROWS), F32),
            pltpu.VMEM((ROWS, COLS), F32),
            pltpu.VMEM((1, ROWS), F32),
            dma((CHIPS,)),
            dma((CHIPS,)),
            dma,
            dma((2, SIDE, SIDE)),
            dma((2, SIDE)),
            dma((4, 9)),
            dma,
            dma,
            dma,
            dma((11,)),
            dma((2,)),
        ],
        compiler_params=pltpu.CompilerParams(
            collective_id=0, has_side_effects=True, vmem_limit_bytes=55040 * 1024
        ),
        name="merge",
    )(expert_grams, expert_weights)
    return merged, ratio[0, 0]


def solution(mesh):
    placed = (P(None, "row", None), P(None, "row", "grp"))
    return jax.shard_map(
        local, mesh=mesh, in_specs=placed, out_specs=(P("row", "grp"), P()), check_vma=False
    )
```

```python
import jax
import jax.numpy as jnp
from jax import lax
from jax.experimental import pallas as pl
from jax.experimental.pallas import tpu as pltpu
from jax.sharding import PartitionSpec as P

MESH = pl.DeviceIdType.MESH
F32, BF16 = jnp.float32, jnp.bfloat16
EXPERTS, ROWS, COLS = 4, 128, 128
CHIPS, SIDE, WIDE, MINE, HALF = 16, 4, 256, 64, 32
GROUP = 4


def split(x):
    high = x.astype(BF16)
    return high, (x - high.astype(F32)).astype(BF16)


def column_sum(x):
    return jnp.sum(x, axis=1, keepdims=True)


def kernel(
    grams, weights, merged, ratio,
    panel, matrix, weights_in, weights_t, partial, partner_part, first, second, outgoing,
    gather_b, gather_0, gather_1, gather_2, residual, mapped_dir, dots, product,
    sums, totals, answer, merged_out, ratio_out,
    panel_sem, partner_sem, matrix_sem, first_sem, second_sem, gather_sem, sums_sem, totals_sem, answer_sem,
    send_sem, local_sem, token_sem,
):
    grp, row = lax.axis_index("grp"), lax.axis_index("row")
    core, chip = lax.rem(row, 2), lax.div(row, 2)
    x, y = lax.div(chip, SIDE), lax.rem(chip, SIDE)
    other = 1 - core

    def at(cx, cy):
        return lax.rem(cx, SIDE) * SIDE + lax.rem(cy, SIDE)

    def device(target):
        return (grp, target * 2 + core)

    partner = (grp, chip * 2 + other)

    def push(src, dst, sent, arrived, to):
        pltpu.make_async_remote_copy(src, dst, sent, arrived, device_id=to, device_id_type=MESH).start()

    def await_bytes(ref, sem):
        pltpu.make_async_copy(ref, ref, sem).wait()

    groups = lax.axis_size("grp")
    barrier = pltpu.get_barrier_semaphore()
    along_z = [(lax.rem(grp + d, groups), row) for d in (2, groups - 2, 1, groups - 1)]
    lines = [device(at(x + d, y)) for d in (2, 1, 3)] + [device(at(x, y + d)) for d in (2, 1, 3)]
    for there in (*along_z, *lines, partner):
        pl.semaphore_signal(barrier, 1, device_id=there, device_id_type=MESH)

    weights_copy = pltpu.make_async_copy(weights, weights_in, local_sem.at[0])
    weights_copy.start()

    def panel_copy(n):
        columns = pl.ds(pl.multiple_of(n * WIDE, WIDE), WIDE)
        return pltpu.make_async_copy(grams.at[:, :, columns], panel.at[n], panel_sem.at[n])

    def fetch(n, _):
        panel_copy(n).start()
        return 0

    lax.fori_loop(0, CHIPS, fetch, 0)

    def tell_z(i):
        for there in along_z:
            pl.semaphore_signal(token_sem.at[i], 1, device_id=there, device_id_type=MESH)

    def hear_z(i):
        pl.semaphore_wait(token_sem.at[i], len(along_z))

    weights_copy.wait()
    turned = jnp.transpose(weights_in[...].reshape(EXPERTS * ROWS, COLS).astype(F32)).astype(BF16)
    weights_t[:, : EXPERTS * ROWS] = turned
    weights_t[:, EXPERTS * ROWS :] = turned

    def compute_panel(target):
        high, low = split(panel[target].reshape(EXPERTS * ROWS, WIDE))
        product = jnp.dot(weights_t[...], jnp.concatenate([high, low], axis=0), preferred_element_type=F32)
        partial[target] = product.reshape(2, MINE, WIDE)
        system = (panel[target, 0] + panel[target, 1]) + (panel[target, 2] + panel[target, 3])
        system_high, system_low = split(system)
        matrix[target, core, 0] = system_high
        matrix[target, core, 1] = system_low

    def panel_step(n, _):
        for i in range(GROUP):
            panel_copy(GROUP * n + i).wait()
        for i in range(GROUP):
            compute_panel(GROUP * n + i)
        return 0

    lax.fori_loop(0, CHIPS // GROUP, panel_step, 0)

    system = (panel[chip, 0] + panel[chip, 1]) + (panel[chip, 2] + panel[chip, 3])
    below = lax.broadcasted_iota(jnp.int32, (ROWS, WIDE), 0) + core * ROWS
    system = system + (below == lax.broadcasted_iota(jnp.int32, (ROWS, WIDE), 1)).astype(F32)
    system_high, system_low = split(system)
    matrix[chip, core, 0] = system_high
    matrix[chip, core, 1] = system_low

    pl.semaphore_wait(barrier, len(along_z) + len(lines) + 1)

    targets = [(2, 2), (1, 2), (3, 2), (2, 1), (2, 3), (1, 1), (3, 1), (1, 3), (3, 3)]
    targets += [(0, 2), (2, 0), (0, 1), (1, 0), (0, 3), (3, 0), (0, 0)]
    for dx, dy in targets:
        target = at(x + dx, y + dy)
        push(partial.at[target, other], partner_part.at[target], send_sem.at[0], partner_sem.at[target], partner)
    for dx, dy in targets:
        target = at(x + dx, y + dy)
        await_bytes(partner_part.at[target], partner_sem.at[target])
        outgoing[target] = partial[target, core] + partner_part[target]
        if dx != 0:
            push(
                outgoing.at[target, pl.ds(0, HALF)], first.at[0, x, lax.rem(y + dy, SIDE)],
                send_sem.at[2], first_sem.at[0, x, lax.rem(y + dy, SIDE)], device(at(x + dx, y)),
            )
        if dy != 0:
            push(
                outgoing.at[target, pl.ds(HALF, HALF)], first.at[1, y, lax.rem(x + dx, SIDE)],
                send_sem.at[2], first_sem.at[1, y, lax.rem(x + dx, SIDE)], device(at(x, y + dy)),
            )

    def first_sum(half, k):
        line, along = (x, y) if half == 0 else (y, x)
        place = lax.rem(along + k, SIDE)
        target = at(x, place) if half == 0 else at(place, y)
        total = outgoing[target, pl.ds(half * HALF, HALF)]
        for j in (1, 3, 2):
            source = lax.rem(line + j, SIDE)
            await_bytes(first.at[half, source, place], first_sem.at[half, source, place])
            total = total + first[half, source, place]
        return total, target

    tell_z(0)

    for k in (2, 1, 3):
        for half in (0, 1):
            along = y if half == 0 else x
            total, target = first_sum(half, k)
            second[half, 0, k] = total
            push(
                second.at[half, 0, k], second.at[half, 1, along],
                send_sem.at[3], second_sem.at[half, along], device(target),
            )
    def send_matrix(target, _):
        push(matrix.at[target, core], matrix.at[target, core], send_sem.at[1], matrix_sem, partner)
        return 0

    lax.fori_loop(0, CHIPS, send_matrix, 0)

    pieces = []
    for half in (0, 1):
        along = y if half == 0 else x
        total, _ = first_sum(half, 0)
        for j in (1, 3, 2):
            source = lax.rem(along + j, SIDE)
            await_bytes(second.at[half, 1, source], second_sem.at[half, source])
            total = total + second[half, 1, source]
        pieces.append(total)
    own_r = jnp.concatenate(pieces, axis=0)

    near_blocks = [(0, 0), (1, 0), (3, 0), (0, 1), (0, 3), (2, 0), (0, 2)]
    middle_blocks = [(1, 1), (1, 3), (3, 1), (3, 3)]
    far_blocks = [(2, 1), (2, 3), (1, 2), (3, 2)]

    def place_of(dx, dy, half):
        if dx != 0 and dy != 0:
            return 9 if (dx, dy) == (2, 2) else 0 if 2 in (dx, dy) else 8
        if half == 0:
            return dx if dy == 0 else 7
        return 3 + dy if dx == 0 else 7

    class Gather:
        def __init__(self, index, buffer):
            self.index, self.buffer = index, buffer

        def send(self, dx, dy, half, ex, ey):
            block = self.buffer.at[at(x + dx, y + dy), half]
            place = place_of((dx - ex) % SIDE, (dy - ey) % SIDE, half)
            push(block, block, send_sem.at[4 + self.index], gather_sem.at[self.index, place], device(at(x + ex, y + ey)))

        def arrive(self, place, ref):
            await_bytes(ref, gather_sem.at[self.index, place])

        def start(self, value):
            buffer = self.buffer
            high, low = split(value)
            for half in (0, 1):
                here = slice(half * HALF, (half + 1) * HALF)
                if self.index < 3:
                    buffer[chip, half, 0] = high[here]
                    buffer[chip, half, 1] = low[here]
                else:
                    buffer[chip, half] = high[here]
            for d in (2, 1, 3):
                self.send(0, 0, 0, d, 0)
                self.send(0, 0, 1, 0, d)

        def start_rest(self):
            for d in (2, 1, 3):
                self.send(0, 0, 0, 0, d)
                self.send(0, 0, 1, d, 0)

        def forward(self):
            half_block = self.buffer.at[0, 0]
            for d in (1, 3, 2):
                self.arrive(d, half_block)
                for e in (2, 1, 3):
                    self.send(d, 0, 0, 0, e)
                self.arrive(3 + d, half_block)
                for e in (2, 1, 3):
                    self.send(0, d, 1, e, 0)

        def near(self):
            self.arrive(7, self.buffer.at[pl.ds(0, 3)])

        def middle(self):
            self.arrive(8, self.buffer.at[pl.ds(0, 4)])

        def far(self):
            self.arrive(0, self.buffer.at[pl.ds(0, 4)])

        def last(self):
            self.arrive(9, self.buffer.at[0])

    def multiply(buffer, planes, blocks):
        places = [at(x + dx, y + dy) for dx, dy in blocks]
        left = jnp.concatenate([buffer[i].reshape(planes * MINE, WIDE) for i in places], axis=1)
        right = jnp.concatenate([matrix[i].reshape(2 * WIDE, WIDE) for i in places], axis=1)
        return lax.dot_general(left, right, (((1,), (1,)), ((), ())), preferred_element_type=F32)

    def fold(total, planes):
        if planes == 2:
            total = total.reshape(2, 2, HALF, 2 * WIDE)
            total = (total[:, 0] + total[:, 1]).reshape(MINE, 2 * WIDE)
        return jnp.concatenate(
            [total[:, i * WIDE : i * WIDE + ROWS] + total[:, i * WIDE + ROWS : (i + 1) * WIDE] for i in (0, 1)],
            axis=1,
        )

    def whole(buffer, planes, origin):
        block = buffer[origin].astype(F32)
        if planes == 2:
            block = block[:, 0] + block[:, 1]
        return block.reshape(MINE, WIDE)

    def products(gather, planes, blocks, first_time):
        for dx, dy in blocks:
            origin = at(x + dx, y + dy)
            block = whole(gather.buffer, planes, origin)
            if first_time:
                residual[origin] = block
                terms = block * block
            else:
                terms = residual[origin] * block
            dots[origin] = terms[:, :ROWS] + terms[:, ROWS:]
        return multiply(gather.buffer, planes, blocks)

    def finish(gather, planes, first_time=False):
        gather.forward()
        gather.near()
        height = planes * MINE
        product[:height] = products(gather, planes, near_blocks, first_time)
        gather.middle()
        product[:height] = product[:height] + products(gather, planes, middle_blocks, first_time)
        gather.far()
        product[:height] = product[:height] + products(gather, planes, far_blocks, first_time)
        gather.last()
        total = product[:height] + products(gather, planes, [(2, 2)], first_time)
        return fold(total, planes), column_sum(jnp.sum(dots[...], axis=0))

    zero = jnp.zeros((MINE, WIDE), F32)

    gather = Gather(0, gather_b)
    gather.start(own_r)
    hear_z(0)
    tell_z(1)
    await_bytes(matrix.at[:, other], matrix_sem)
    gather.start_rest()
    own_w, norm = finish(gather, 2, True)
    initial = norm

    alpha = beta = None
    own_p = own_s = own_t = own_x = None
    for step, (buffer, planes) in enumerate(((gather_0, 2), (gather_1, 2), (gather_2, 1))):
        gather = Gather(step + 1, buffer)
        gather.start(own_w)
        if step > 0:
            before, before_planes = ((gather_0, 2), (gather_1, 2))[step - 1]

            def advance(origin, total, buffer=before, planes=before_planes, step=step, alpha=alpha, beta=old_beta):
                direction = whole(buffer, planes, origin)
                if step > 1:
                    direction = direction + beta * mapped_dir[origin]
                mapped_dir[origin] = direction
                block = residual[origin] - alpha * direction
                residual[origin] = block
                return total + block * block

            following = column_sum(lax.fori_loop(0, CHIPS, advance, zero))
            beta = following / norm
            norm = following
        gather.start_rest()
        own_u, overlap = finish(gather, planes)
        if step == 0:
            alpha = norm / overlap
            own_p, own_s, own_t = own_r, own_w, own_u
            own_x = alpha * own_p
        else:
            alpha = norm / (overlap - beta * norm / alpha)
            own_p = own_r + beta * own_p
            own_s = own_w + beta * own_s
            own_t = own_u + beta * own_t
            own_x = own_x + alpha * own_p
        old_beta = beta
        own_r = own_r - alpha * own_s
        own_w = own_w - alpha * own_t

    def last_advance(origin, total):
        direction = whole(gather_2, 1, origin) + beta * mapped_dir[origin]
        block = residual[origin] - alpha * direction
        return total + block * block

    following = column_sum(lax.fori_loop(0, CHIPS, last_advance, zero))
    beta = following / norm
    norm = following

    own_s = own_w + beta * own_s
    own_p = own_r + beta * own_p
    close = own_r - alpha * own_s
    lane = lax.broadcasted_iota(jnp.int32, (MINE, ROWS), 1)
    def lay_flat(columns):
        packed = jnp.zeros((MINE, ROWS), F32)
        for i, column in enumerate(columns):
            packed = jnp.where(lane == i, column, packed)
        return jnp.transpose(jnp.concatenate([packed, jnp.zeros_like(packed)], axis=0))[: len(columns)]

    sums[chip] = lay_flat([column_sum(t) for t in (own_r * own_w, close * close, close * own_s, own_s * own_s)])

    def tell_chip(n, _):
        push(sums.at[chip], sums.at[chip], send_sem.at[8], sums_sem, device(lax.rem(chip + n, CHIPS)))
        return 0

    lax.fori_loop(1, CHIPS, tell_chip, 0)
    hear_z(1)
    known = lay_flat([norm, beta, alpha, initial])
    used = lax.broadcasted_iota(jnp.int32, (1, ROWS), 1) < MINE
    norm, beta, alpha, initial = (jnp.where(used, known[i : i + 1], 1.0) for i in range(4))
    await_bytes(sums.at[pl.ds(0, CHIPS - 1)], sums_sem)
    gathered = jnp.where(used, jnp.sum(sums[...], axis=0), 1.0)
    overlap, close_close, close_s, s_s = (gathered[i : i + 1] for i in range(4))
    last = norm / jnp.where(used, overlap - beta * norm / alpha, 1.0)
    excess = last - alpha
    final = jnp.maximum(close_close - 2.0 * excess * close_s + excess * excess * s_s, 0.0)

    place = grp * 2 + core
    final = column_sum(jnp.where(used, final, 0.0))
    initial = column_sum(jnp.where(used, initial, 0.0))
    totals[place] = jnp.where(lax.broadcasted_iota(jnp.int32, (1, ROWS), 1) == 0, final, initial)

    def tell_group(n, _):
        there = lax.rem(place + n, 2 * groups)
        push(
            totals.at[place], totals.at[place], send_sem.at[10], totals_sem,
            (lax.div(there, 2), chip * 2 + lax.rem(there, 2)),
        )
        return 0

    lax.fori_loop(1, 2 * groups, tell_group, 0)
    last = jnp.transpose(jnp.broadcast_to(last, (ROWS, ROWS)))[:MINE, :1]
    own_x = own_x + last * own_p
    answer[core, 0] = own_x[:, :ROWS]
    answer[core, 1] = own_x[:, ROWS:]
    push(answer.at[core, other], answer.at[core, other], send_sem.at[9], answer_sem, partner)
    await_bytes(answer.at[other, core], answer_sem)
    merged_out[...] = jnp.transpose(jnp.concatenate([answer[0, core], answer[1, core]], axis=0))
    merged_copy = pltpu.make_async_copy(merged_out, merged, local_sem.at[1])
    merged_copy.start()

    await_bytes(partner_part, send_sem.at[0])
    await_bytes(matrix.at[:, 0], send_sem.at[1])
    await_bytes(first.at[:, pl.ds(0, 3)], send_sem.at[2])
    await_bytes(second.at[:, 0, pl.ds(0, 3)], send_sem.at[3])
    for i, buffer in enumerate((gather_b, gather_0, gather_1, gather_2)):
        await_bytes(buffer.at[pl.ds(0, CHIPS - 1)], send_sem.at[4 + i])
    await_bytes(sums.at[pl.ds(0, CHIPS - 1)], send_sem.at[8])
    await_bytes(answer.at[0, 0], send_sem.at[9])
    await_bytes(totals.at[pl.ds(0, 2 * groups - 1)], send_sem.at[10])
    merged_copy.wait()
    await_bytes(totals.at[pl.ds(0, 2 * groups - 1)], totals_sem)
    over_all = jnp.sum(totals[...], axis=0)
    ratio_out[...] = jnp.sqrt(over_all[:, 0:1] / over_all[:, 1:2]) + jnp.zeros((1, ROWS), F32)
    ratio_copy = pltpu.make_async_copy(ratio_out, ratio, local_sem.at[0])
    ratio_copy.start()
    ratio_copy.wait()


def local(expert_grams, expert_weights):
    groups = lax.axis_size("grp")
    hbm = pl.BlockSpec(memory_space=pltpu.HBM)
    anywhere = pl.BlockSpec(memory_space=pl.ANY)
    dma = pltpu.SemaphoreType.DMA
    merged, ratio = pl.pallas_call(
        kernel,
        out_shape=(jax.ShapeDtypeStruct((ROWS, COLS), F32), jax.ShapeDtypeStruct((1, ROWS), F32)),
        in_specs=[hbm, hbm],
        out_specs=(anywhere, anywhere),
        scratch_shapes=[
            pltpu.VMEM((CHIPS, EXPERTS, ROWS, WIDE), F32),
            pltpu.VMEM((CHIPS, 2, 2, ROWS, WIDE), BF16),
            pltpu.VMEM((EXPERTS, ROWS, COLS), BF16),
            pltpu.VMEM((COLS, 2 * EXPERTS * ROWS), BF16),
            pltpu.VMEM((CHIPS, 2, MINE, WIDE), F32),
            pltpu.VMEM((CHIPS, MINE, WIDE), F32),
            pltpu.VMEM((2, SIDE, SIDE, HALF, WIDE), F32),
            pltpu.VMEM((2, 2, SIDE, HALF, WIDE), F32),
            pltpu.VMEM((CHIPS, MINE, WIDE), F32),
            pltpu.VMEM((CHIPS, 2, 2, HALF, WIDE), BF16),
            pltpu.VMEM((CHIPS, 2, 2, HALF, WIDE), BF16),
            pltpu.VMEM((CHIPS, 2, 2, HALF, WIDE), BF16),
            pltpu.VMEM((CHIPS, 2, HALF, WIDE), BF16),
            pltpu.VMEM((CHIPS, MINE, WIDE), F32),
            pltpu.VMEM((CHIPS, MINE, WIDE), F32),
            pltpu.VMEM((CHIPS, MINE, ROWS), F32),
            pltpu.VMEM((2 * MINE, 2 * WIDE), F32),
            pltpu.VMEM((CHIPS, 4, ROWS), F32),
            pltpu.VMEM((2 * groups, 1, ROWS), F32),
            pltpu.VMEM((2, 2, MINE, ROWS), F32),
            pltpu.VMEM((ROWS, COLS), F32),
            pltpu.VMEM((1, ROWS), F32),
            dma((CHIPS,)),
            dma((CHIPS,)),
            dma,
            dma((2, SIDE, SIDE)),
            dma((2, SIDE)),
            dma((4, 10)),
            dma,
            dma,
            dma,
            dma((11,)),
            dma((2,)),
            pltpu.SemaphoreType.REGULAR((2,)),
        ],
        compiler_params=pltpu.CompilerParams(
            collective_id=0, has_side_effects=True, vmem_limit_bytes=55040 * 1024
        ),
        name="merge",
    )(expert_grams, expert_weights)
    return merged, ratio[0, 0]


def solution(mesh):
    placed = (P(None, "row", None), P(None, "row", "grp"))
    return jax.shard_map(
        local, mesh=mesh, in_specs=placed, out_specs=(P("row", "grp"), P()), check_vma=False
    )
```

```python
import jax
import jax.numpy as jnp
from jax import lax
from jax.experimental import pallas as pl
from jax.experimental.pallas import tpu as pltpu
from jax.sharding import PartitionSpec as P

MESH = pl.DeviceIdType.MESH
F32, BF16 = jnp.float32, jnp.bfloat16
EXPERTS, ROWS, COLS = 4, 128, 128
CHIPS, SIDE, WIDE, MINE, HALF = 16, 4, 256, 64, 32
GROUP, BEFORE = 4, 0


def split(x):
    high = x.astype(BF16)
    return high, (x - high.astype(F32)).astype(BF16)


def column_sum(x):
    return jnp.sum(x, axis=1, keepdims=True)


def kernel(
    grams, weights, merged, ratio,
    panel, matrix, weights_in, weights_t, partial, partner_part, first, second, outgoing,
    gather_b, gather_0, gather_1, gather_2, residual, mapped_dir, dots, product,
    sums, totals, answer, merged_out, ratio_out,
    panel_sem, partner_sem, matrix_sem, first_sem, second_sem, gather_sem, sums_sem, totals_sem, answer_sem,
    send_sem, local_sem, token_sem,
):
    grp, row = lax.axis_index("grp"), lax.axis_index("row")
    core, chip = lax.rem(row, 2), lax.div(row, 2)
    x, y = lax.div(chip, SIDE), lax.rem(chip, SIDE)
    other = 1 - core

    def at(cx, cy):
        return lax.rem(cx, SIDE) * SIDE + lax.rem(cy, SIDE)

    def device(target):
        return (grp, target * 2 + core)

    partner = (grp, chip * 2 + other)

    def push(src, dst, sent, arrived, to):
        pltpu.make_async_remote_copy(src, dst, sent, arrived, device_id=to, device_id_type=MESH).start()

    def await_bytes(ref, sem):
        pltpu.make_async_copy(ref, ref, sem).wait()

    groups = lax.axis_size("grp")
    barrier = pltpu.get_barrier_semaphore()
    along_z = [(lax.rem(grp + d, groups), row) for d in (2, groups - 2, 1, groups - 1)]
    lines = [device(at(x + d, y)) for d in (2, 1, 3)] + [device(at(x, y + d)) for d in (2, 1, 3)]
    order = [(2, 2), (1, 2), (3, 2), (2, 1), (2, 3), (1, 1), (3, 1), (1, 3), (3, 3)]
    order += [(0, 2), (2, 0), (0, 1), (1, 0), (0, 3), (3, 0), (0, 0)]
    targets = [at(x + dx, y + dy) for dx, dy in order]

    def panel_copy(n):
        columns = pl.ds(pl.multiple_of(targets[n] * WIDE, WIDE), WIDE)
        return pltpu.make_async_copy(grams.at[:, :, columns], panel.at[n], panel_sem.at[n])

    weights_copy = pltpu.make_async_copy(weights, weights_in, local_sem.at[0])
    weights_copy.start()
    for n in range(GROUP):
        panel_copy(n).start()
    for there in (*along_z, *lines, partner):
        pl.semaphore_signal(barrier, 1, device_id=there, device_id_type=MESH)
    for n in range(GROUP, CHIPS):
        panel_copy(n).start()

    def tell_z(i):
        for there in along_z:
            pl.semaphore_signal(token_sem.at[i], 1, device_id=there, device_id_type=MESH)

    def hear_z(i):
        pl.semaphore_wait(token_sem.at[i], len(along_z))

    weights_copy.wait()
    turned = jnp.transpose(weights_in[...].reshape(EXPERTS * ROWS, COLS).astype(F32)).astype(BF16)
    weights_t[:, : EXPERTS * ROWS] = turned
    weights_t[:, EXPERTS * ROWS :] = turned

    def compute_panel(n):
        target = targets[n]
        high, low = split(panel[n].reshape(EXPERTS * ROWS, WIDE))
        product = jnp.dot(weights_t[...], jnp.concatenate([high, low], axis=0), preferred_element_type=F32)
        partial[target] = product.reshape(2, MINE, WIDE)
        system = (panel[n, 0] + panel[n, 1]) + (panel[n, 2] + panel[n, 3])
        if order[n] == (0, 0):
            below = lax.broadcasted_iota(jnp.int32, (ROWS, WIDE), 0) + core * ROWS
            system = system + (below == lax.broadcasted_iota(jnp.int32, (ROWS, WIDE), 1)).astype(F32)
        system_high, system_low = split(system)
        matrix[target, core, 0] = system_high
        matrix[target, core, 1] = system_low

    def swap_panel(n):
        target = targets[n]
        push(partial.at[target, other], partner_part.at[target], send_sem.at[0], partner_sem.at[target], partner)

    def forward_panel(n):
        (dx, dy), target = order[n], targets[n]
        await_bytes(partner_part.at[target], partner_sem.at[target])
        outgoing[target] = partial[target, core] + partner_part[target]
        if dx != 0:
            push(
                outgoing.at[target, pl.ds(0, HALF)], first.at[0, x, lax.rem(y + dy, SIDE)],
                send_sem.at[2], first_sem.at[0, x, lax.rem(y + dy, SIDE)], device(at(x + dx, y)),
            )
        if dy != 0:
            push(
                outgoing.at[target, pl.ds(HALF, HALF)], first.at[1, y, lax.rem(x + dx, SIDE)],
                send_sem.at[2], first_sem.at[1, y, lax.rem(x + dx, SIDE)], device(at(x, y + dy)),
            )

    def compute_group(group):
        for n in group:
            panel_copy(n).wait()
        for n in group:
            compute_panel(n)

    groups_of_panels = [range(i, i + GROUP) for i in range(0, CHIPS, GROUP)]
    for i, group in enumerate(groups_of_panels):
        compute_group(group)
        if i == BEFORE:
            pl.semaphore_wait(barrier, len(along_z) + len(lines) + 1)
            for earlier in groups_of_panels[:BEFORE]:
                for n in earlier:
                    swap_panel(n)
        if i >= BEFORE:
            for n in group:
                swap_panel(n)
        if i > BEFORE:
            for n in groups_of_panels[i - BEFORE - 1]:
                forward_panel(n)
    for group in groups_of_panels[len(groups_of_panels) - BEFORE - 1 :]:
        for n in group:
            forward_panel(n)

    def first_sum(half, k):
        line, along = (x, y) if half == 0 else (y, x)
        place = lax.rem(along + k, SIDE)
        target = at(x, place) if half == 0 else at(place, y)
        total = outgoing[target, pl.ds(half * HALF, HALF)]
        for j in (1, 3, 2):
            source = lax.rem(line + j, SIDE)
            await_bytes(first.at[half, source, place], first_sem.at[half, source, place])
            total = total + first[half, source, place]
        return total, target

    tell_z(0)

    for k in (2, 1, 3):
        for half in (0, 1):
            along = y if half == 0 else x
            total, target = first_sum(half, k)
            second[half, 0, k] = total
            push(
                second.at[half, 0, k], second.at[half, 1, along],
                send_sem.at[3], second_sem.at[half, along], device(target),
            )
    def send_matrix(target, _):
        push(matrix.at[target, core], matrix.at[target, core], send_sem.at[1], matrix_sem, partner)
        return 0

    lax.fori_loop(0, CHIPS, send_matrix, 0)

    pieces = []
    for half in (0, 1):
        along = y if half == 0 else x
        total, _ = first_sum(half, 0)
        for j in (1, 3, 2):
            source = lax.rem(along + j, SIDE)
            await_bytes(second.at[half, 1, source], second_sem.at[half, source])
            total = total + second[half, 1, source]
        pieces.append(total)
    own_r = jnp.concatenate(pieces, axis=0)

    near_blocks = [(0, 0), (1, 0), (3, 0), (0, 1), (0, 3), (2, 0), (0, 2)]
    middle_blocks = [(1, 1), (1, 3), (3, 1), (3, 3)]
    far_blocks = [(2, 1), (2, 3), (1, 2), (3, 2)]

    def place_of(dx, dy, half):
        if dx != 0 and dy != 0:
            return 9 if (dx, dy) == (2, 2) else 0 if 2 in (dx, dy) else 8
        if half == 0:
            return dx if dy == 0 else 7
        return 3 + dy if dx == 0 else 7

    class Gather:
        def __init__(self, index, buffer):
            self.index, self.buffer = index, buffer

        def send(self, dx, dy, half, ex, ey):
            block = self.buffer.at[at(x + dx, y + dy), half]
            place = place_of((dx - ex) % SIDE, (dy - ey) % SIDE, half)
            push(block, block, send_sem.at[4 + self.index], gather_sem.at[self.index, place], device(at(x + ex, y + ey)))

        def arrive(self, place, ref):
            await_bytes(ref, gather_sem.at[self.index, place])

        def start(self, value):
            buffer = self.buffer
            high, low = split(value)
            for half in (0, 1):
                here = slice(half * HALF, (half + 1) * HALF)
                if self.index < 3:
                    buffer[chip, half, 0] = high[here]
                    buffer[chip, half, 1] = low[here]
                else:
                    buffer[chip, half] = high[here]
            for d in (2, 1, 3):
                self.send(0, 0, 0, d, 0)
                self.send(0, 0, 1, 0, d)

        def start_rest(self):
            for d in (2, 1, 3):
                self.send(0, 0, 0, 0, d)
                self.send(0, 0, 1, d, 0)

        def forward(self):
            half_block = self.buffer.at[0, 0]
            for d in (1, 3, 2):
                self.arrive(d, half_block)
                for e in (2, 1, 3):
                    self.send(d, 0, 0, 0, e)
                self.arrive(3 + d, half_block)
                for e in (2, 1, 3):
                    self.send(0, d, 1, e, 0)

        def near(self):
            self.arrive(7, self.buffer.at[pl.ds(0, 3)])

        def middle(self):
            self.arrive(8, self.buffer.at[pl.ds(0, 4)])

        def far(self):
            self.arrive(0, self.buffer.at[pl.ds(0, 4)])

        def last(self):
            self.arrive(9, self.buffer.at[0])

    def multiply(buffer, planes, blocks):
        places = [at(x + dx, y + dy) for dx, dy in blocks]
        left = jnp.concatenate([buffer[i].reshape(planes * MINE, WIDE) for i in places], axis=1)
        right = jnp.concatenate([matrix[i].reshape(2 * WIDE, WIDE) for i in places], axis=1)
        return lax.dot_general(left, right, (((1,), (1,)), ((), ())), preferred_element_type=F32)

    def fold(total, planes):
        if planes == 2:
            total = total.reshape(2, 2, HALF, 2 * WIDE)
            total = (total[:, 0] + total[:, 1]).reshape(MINE, 2 * WIDE)
        return jnp.concatenate(
            [total[:, i * WIDE : i * WIDE + ROWS] + total[:, i * WIDE + ROWS : (i + 1) * WIDE] for i in (0, 1)],
            axis=1,
        )

    def whole(buffer, planes, origin):
        block = buffer[origin].astype(F32)
        if planes == 2:
            block = block[:, 0] + block[:, 1]
        return block.reshape(MINE, WIDE)

    def products(gather, planes, blocks, first_time):
        for dx, dy in blocks:
            origin = at(x + dx, y + dy)
            block = whole(gather.buffer, planes, origin)
            if first_time:
                residual[origin] = block
                terms = block * block
            else:
                terms = residual[origin] * block
            dots[origin] = terms[:, :ROWS] + terms[:, ROWS:]
        return multiply(gather.buffer, planes, blocks)

    def finish(gather, planes, first_time=False):
        gather.forward()
        gather.near()
        height = planes * MINE
        product[:height] = products(gather, planes, near_blocks, first_time)
        gather.middle()
        product[:height] = product[:height] + products(gather, planes, middle_blocks, first_time)
        gather.far()
        product[:height] = product[:height] + products(gather, planes, far_blocks, first_time)
        gather.last()
        total = product[:height] + products(gather, planes, [(2, 2)], first_time)
        return fold(total, planes), column_sum(jnp.sum(dots[...], axis=0))

    zero = jnp.zeros((MINE, WIDE), F32)

    gather = Gather(0, gather_b)
    gather.start(own_r)
    hear_z(0)
    tell_z(1)
    await_bytes(matrix.at[:, other], matrix_sem)
    gather.start_rest()
    own_w, norm = finish(gather, 2, True)
    initial = norm

    alpha = beta = None
    own_p = own_s = own_t = own_x = None
    for step, (buffer, planes) in enumerate(((gather_0, 2), (gather_1, 2), (gather_2, 1))):
        gather = Gather(step + 1, buffer)
        gather.start(own_w)
        if step > 0:
            before, before_planes = ((gather_0, 2), (gather_1, 2))[step - 1]

            def advance(origin, total, buffer=before, planes=before_planes, step=step, alpha=alpha, beta=old_beta):
                direction = whole(buffer, planes, origin)
                if step > 1:
                    direction = direction + beta * mapped_dir[origin]
                mapped_dir[origin] = direction
                block = residual[origin] - alpha * direction
                residual[origin] = block
                return total + block * block

            following = column_sum(lax.fori_loop(0, CHIPS, advance, zero))
            beta = following / norm
            norm = following
        gather.start_rest()
        own_u, overlap = finish(gather, planes)
        if step == 0:
            alpha = norm / overlap
            own_p, own_s, own_t = own_r, own_w, own_u
            own_x = alpha * own_p
        else:
            alpha = norm / (overlap - beta * norm / alpha)
            own_p = own_r + beta * own_p
            own_s = own_w + beta * own_s
            own_t = own_u + beta * own_t
            own_x = own_x + alpha * own_p
        old_beta = beta
        own_r = own_r - alpha * own_s
        own_w = own_w - alpha * own_t

    def last_advance(origin, total):
        direction = whole(gather_2, 1, origin) + beta * mapped_dir[origin]
        block = residual[origin] - alpha * direction
        return total + block * block

    following = column_sum(lax.fori_loop(0, CHIPS, last_advance, zero))
    beta = following / norm
    norm = following

    own_s = own_w + beta * own_s
    own_p = own_r + beta * own_p
    close = own_r - alpha * own_s
    lane = lax.broadcasted_iota(jnp.int32, (MINE, ROWS), 1)
    def lay_flat(columns):
        packed = jnp.zeros((MINE, ROWS), F32)
        for i, column in enumerate(columns):
            packed = jnp.where(lane == i, column, packed)
        return jnp.transpose(jnp.concatenate([packed, jnp.zeros_like(packed)], axis=0))[: len(columns)]

    sums[chip] = lay_flat([column_sum(t) for t in (own_r * own_w, close * close, close * own_s, own_s * own_s)])

    def tell_chip(n, _):
        push(sums.at[chip], sums.at[chip], send_sem.at[8], sums_sem, device(lax.rem(chip + n, CHIPS)))
        return 0

    lax.fori_loop(1, CHIPS, tell_chip, 0)
    hear_z(1)
    known = lay_flat([norm, beta, alpha, initial])
    used = lax.broadcasted_iota(jnp.int32, (1, ROWS), 1) < MINE
    norm, beta, alpha, initial = (jnp.where(used, known[i : i + 1], 1.0) for i in range(4))
    await_bytes(sums.at[pl.ds(0, CHIPS - 1)], sums_sem)
    gathered = jnp.where(used, jnp.sum(sums[...], axis=0), 1.0)
    overlap, close_close, close_s, s_s = (gathered[i : i + 1] for i in range(4))
    last = norm / jnp.where(used, overlap - beta * norm / alpha, 1.0)
    excess = last - alpha
    final = jnp.maximum(close_close - 2.0 * excess * close_s + excess * excess * s_s, 0.0)

    place = grp * 2 + core
    final = column_sum(jnp.where(used, final, 0.0))
    initial = column_sum(jnp.where(used, initial, 0.0))
    totals[place] = jnp.where(lax.broadcasted_iota(jnp.int32, (1, ROWS), 1) == 0, final, initial)

    def tell_group(n, _):
        there = lax.rem(place + n, 2 * groups)
        push(
            totals.at[place], totals.at[place], send_sem.at[10], totals_sem,
            (lax.div(there, 2), chip * 2 + lax.rem(there, 2)),
        )
        return 0

    lax.fori_loop(1, 2 * groups, tell_group, 0)
    last = jnp.transpose(jnp.broadcast_to(last, (ROWS, ROWS)))[:MINE, :1]
    own_x = own_x + last * own_p
    answer[core, 0] = own_x[:, :ROWS]
    answer[core, 1] = own_x[:, ROWS:]
    push(answer.at[core, other], answer.at[core, other], send_sem.at[9], answer_sem, partner)
    await_bytes(answer.at[other, core], answer_sem)
    merged_out[...] = jnp.transpose(jnp.concatenate([answer[0, core], answer[1, core]], axis=0))
    merged_copy = pltpu.make_async_copy(merged_out, merged, local_sem.at[1])
    merged_copy.start()

    await_bytes(partner_part, send_sem.at[0])
    await_bytes(matrix.at[:, 0], send_sem.at[1])
    await_bytes(first.at[:, pl.ds(0, 3)], send_sem.at[2])
    await_bytes(second.at[:, 0, pl.ds(0, 3)], send_sem.at[3])
    for i, buffer in enumerate((gather_b, gather_0, gather_1, gather_2)):
        await_bytes(buffer.at[pl.ds(0, CHIPS - 1)], send_sem.at[4 + i])
    await_bytes(sums.at[pl.ds(0, CHIPS - 1)], send_sem.at[8])
    await_bytes(answer.at[0, 0], send_sem.at[9])
    await_bytes(totals.at[pl.ds(0, 2 * groups - 1)], send_sem.at[10])
    merged_copy.wait()
    await_bytes(totals.at[pl.ds(0, 2 * groups - 1)], totals_sem)
    over_all = jnp.sum(totals[...], axis=0)
    ratio_out[...] = jnp.sqrt(over_all[:, 0:1] / over_all[:, 1:2]) + jnp.zeros((1, ROWS), F32)
    ratio_copy = pltpu.make_async_copy(ratio_out, ratio, local_sem.at[0])
    ratio_copy.start()
    ratio_copy.wait()


def local(expert_grams, expert_weights):
    groups = lax.axis_size("grp")
    hbm = pl.BlockSpec(memory_space=pltpu.HBM)
    anywhere = pl.BlockSpec(memory_space=pl.ANY)
    dma = pltpu.SemaphoreType.DMA
    merged, ratio = pl.pallas_call(
        kernel,
        out_shape=(jax.ShapeDtypeStruct((ROWS, COLS), F32), jax.ShapeDtypeStruct((1, ROWS), F32)),
        in_specs=[hbm, hbm],
        out_specs=(anywhere, anywhere),
        scratch_shapes=[
            pltpu.VMEM((CHIPS, EXPERTS, ROWS, WIDE), F32),
            pltpu.VMEM((CHIPS, 2, 2, ROWS, WIDE), BF16),
            pltpu.VMEM((EXPERTS, ROWS, COLS), BF16),
            pltpu.VMEM((COLS, 2 * EXPERTS * ROWS), BF16),
            pltpu.VMEM((CHIPS, 2, MINE, WIDE), F32),
            pltpu.VMEM((CHIPS, MINE, WIDE), F32),
            pltpu.VMEM((2, SIDE, SIDE, HALF, WIDE), F32),
            pltpu.VMEM((2, 2, SIDE, HALF, WIDE), F32),
            pltpu.VMEM((CHIPS, MINE, WIDE), F32),
            pltpu.VMEM((CHIPS, 2, 2, HALF, WIDE), BF16),
            pltpu.VMEM((CHIPS, 2, 2, HALF, WIDE), BF16),
            pltpu.VMEM((CHIPS, 2, 2, HALF, WIDE), BF16),
            pltpu.VMEM((CHIPS, 2, HALF, WIDE), BF16),
            pltpu.VMEM((CHIPS, MINE, WIDE), F32),
            pltpu.VMEM((CHIPS, MINE, WIDE), F32),
            pltpu.VMEM((CHIPS, MINE, ROWS), F32),
            pltpu.VMEM((2 * MINE, 2 * WIDE), F32),
            pltpu.VMEM((CHIPS, 4, ROWS), F32),
            pltpu.VMEM((2 * groups, 1, ROWS), F32),
            pltpu.VMEM((2, 2, MINE, ROWS), F32),
            pltpu.VMEM((ROWS, COLS), F32),
            pltpu.VMEM((1, ROWS), F32),
            dma((CHIPS,)),
            dma((CHIPS,)),
            dma,
            dma((2, SIDE, SIDE)),
            dma((2, SIDE)),
            dma((4, 10)),
            dma,
            dma,
            dma,
            dma((11,)),
            dma((2,)),
            pltpu.SemaphoreType.REGULAR((2,)),
        ],
        compiler_params=pltpu.CompilerParams(
            collective_id=0, has_side_effects=True, vmem_limit_bytes=55040 * 1024
        ),
        name="merge",
    )(expert_grams, expert_weights)
    return merged, ratio[0, 0]


def solution(mesh):
    placed = (P(None, "row", None), P(None, "row", "grp"))
    return jax.shard_map(
        local, mesh=mesh, in_specs=placed, out_specs=(P("row", "grp"), P()), check_vma=False
    )
```

```python
import jax
import jax.numpy as jnp
from jax import lax
from jax.experimental import pallas as pl
from jax.experimental.pallas import tpu as pltpu
from jax.sharding import PartitionSpec as P

MESH = pl.DeviceIdType.MESH
F32, BF16 = jnp.float32, jnp.bfloat16
EXPERTS, ROWS, COLS = 4, 128, 128
CHIPS, SIDE, WIDE, MINE, HALF = 16, 4, 256, 64, 32
GROUP, BEFORE = 2, 0


def split(x):
    high = x.astype(BF16)
    return high, (x - high.astype(F32)).astype(BF16)


def column_sum(x):
    return jnp.sum(x, axis=1, keepdims=True)


def kernel(
    grams, weights, merged, ratio,
    panel, matrix, weights_in, weights_t, partial, partner_part, first, second, outgoing,
    gather_b, gather_0, gather_1, gather_2, residual, mapped_dir, dots, product,
    sums, totals, answer,
    panel_sem, partner_sem, matrix_sem, first_sem, second_sem, gather_sem, sums_sem, totals_sem, answer_sem,
    send_sem, local_sem, token_sem,
):
    grp, row = lax.axis_index("grp"), lax.axis_index("row")
    core, chip = lax.rem(row, 2), lax.div(row, 2)
    x, y = lax.div(chip, SIDE), lax.rem(chip, SIDE)
    other = 1 - core

    def at(cx, cy):
        return lax.rem(cx, SIDE) * SIDE + lax.rem(cy, SIDE)

    def device(target):
        return (grp, target * 2 + core)

    partner = (grp, chip * 2 + other)

    def push(src, dst, sent, arrived, to):
        pltpu.make_async_remote_copy(src, dst, sent, arrived, device_id=to, device_id_type=MESH).start()

    def await_bytes(ref, sem):
        pltpu.make_async_copy(ref, ref, sem).wait()

    groups = lax.axis_size("grp")
    barrier = pltpu.get_barrier_semaphore()
    along_z = [(lax.rem(grp + d, groups), row) for d in (2, groups - 2, 1, groups - 1)]
    lines = [device(at(x + d, y)) for d in (2, 1, 3)] + [device(at(x, y + d)) for d in (2, 1, 3)]
    order = [(2, 2), (1, 2), (3, 2), (2, 1), (2, 3), (1, 1), (3, 1), (1, 3), (3, 3)]
    order += [(0, 2), (2, 0), (0, 1), (1, 0), (0, 3), (3, 0), (0, 0)]
    targets = [at(x + dx, y + dy) for dx, dy in order]

    def panel_copy(n):
        columns = pl.ds(pl.multiple_of(targets[n] * WIDE, WIDE), WIDE)
        return pltpu.make_async_copy(grams.at[:, :, columns], panel.at[n], panel_sem.at[n // GROUP])

    weights_copy = pltpu.make_async_copy(weights, weights_in, local_sem.at[0])
    weights_copy.start()
    for n in range(GROUP):
        panel_copy(n).start()
    for there in (*along_z, *lines, partner):
        pl.semaphore_signal(barrier, 1, device_id=there, device_id_type=MESH)
    for n in range(GROUP, CHIPS):
        panel_copy(n).start()

    def tell_z(i):
        for there in along_z:
            pl.semaphore_signal(token_sem.at[i], 1, device_id=there, device_id_type=MESH)

    def hear_z(i):
        pl.semaphore_wait(token_sem.at[i], len(along_z))

    weights_copy.wait()
    turned = jnp.transpose(weights_in[...].reshape(EXPERTS * ROWS, COLS).astype(F32)).astype(BF16)
    weights_t[:, : EXPERTS * ROWS] = turned
    weights_t[:, EXPERTS * ROWS :] = turned

    def compute_panel(n):
        target = targets[n]
        high, low = split(panel[n].reshape(EXPERTS * ROWS, WIDE))
        product = jnp.dot(weights_t[...], jnp.concatenate([high, low], axis=0), preferred_element_type=F32)
        partial[target] = product.reshape(2, MINE, WIDE)
        system = (panel[n, 0] + panel[n, 1]) + (panel[n, 2] + panel[n, 3])
        if order[n] == (0, 0):
            below = lax.broadcasted_iota(jnp.int32, (ROWS, WIDE), 0) + core * ROWS
            system = system + (below == lax.broadcasted_iota(jnp.int32, (ROWS, WIDE), 1)).astype(F32)
        system_high, system_low = split(system)
        matrix[target, core, 0] = system_high
        matrix[target, core, 1] = system_low

    def swap_panel(n):
        target = targets[n]
        push(partial.at[target, other], partner_part.at[target], send_sem.at[0], partner_sem.at[n // GROUP], partner)

    def forward_panel(n):
        (dx, dy), target = order[n], targets[n]
        if n % GROUP == 0:
            await_bytes(partner_part.at[pl.ds(0, GROUP)], partner_sem.at[n // GROUP])
        outgoing[target] = partial[target, core] + partner_part[target]
        if dx != 0:
            push(
                outgoing.at[target, pl.ds(0, HALF)], first.at[0, x, lax.rem(y + dy, SIDE)],
                send_sem.at[2], first_sem.at[0, lax.rem(y + dy, SIDE)], device(at(x + dx, y)),
            )
        if dy != 0:
            push(
                outgoing.at[target, pl.ds(HALF, HALF)], first.at[1, y, lax.rem(x + dx, SIDE)],
                send_sem.at[2], first_sem.at[1, lax.rem(x + dx, SIDE)], device(at(x, y + dy)),
            )

    def compute_group(group):
        await_bytes(panel.at[pl.ds(0, GROUP)], panel_sem.at[group[0] // GROUP])
        for n in group:
            compute_panel(n)

    groups_of_panels = [range(i, i + GROUP) for i in range(0, CHIPS, GROUP)]
    for i, group in enumerate(groups_of_panels):
        compute_group(group)
        if i == BEFORE:
            pl.semaphore_wait(barrier, len(along_z) + len(lines) + 1)
            for earlier in groups_of_panels[:BEFORE]:
                for n in earlier:
                    swap_panel(n)
        if i >= BEFORE:
            for n in group:
                swap_panel(n)
        if i > BEFORE:
            for n in groups_of_panels[i - BEFORE - 1]:
                forward_panel(n)
    for group in groups_of_panels[len(groups_of_panels) - BEFORE - 1 :]:
        for n in group:
            forward_panel(n)

    def first_sum(half, k):
        line, along = (x, y) if half == 0 else (y, x)
        place = lax.rem(along + k, SIDE)
        target = at(x, place) if half == 0 else at(place, y)
        total = outgoing[target, pl.ds(half * HALF, HALF)]
        await_bytes(first.at[half, pl.ds(0, SIDE - 1), 0], first_sem.at[half, place])
        for j in (1, 3, 2):
            total = total + first[half, lax.rem(line + j, SIDE), place]
        return total, target

    tell_z(0)

    for k in (2, 1, 3):
        for half in (0, 1):
            along = y if half == 0 else x
            total, target = first_sum(half, k)
            second[half, 0, k] = total
            push(
                second.at[half, 0, k], second.at[half, 1, along],
                send_sem.at[3], second_sem.at[half], device(target),
            )
    def send_matrix(target, _):
        push(matrix.at[target, core], matrix.at[target, core], send_sem.at[1], matrix_sem, partner)
        return 0

    lax.fori_loop(0, CHIPS, send_matrix, 0)

    pieces = []
    for half in (0, 1):
        along = y if half == 0 else x
        total, _ = first_sum(half, 0)
        await_bytes(second.at[half, 1, pl.ds(0, SIDE - 1)], second_sem.at[half])
        for j in (1, 3, 2):
            total = total + second[half, 1, lax.rem(along + j, SIDE)]
        pieces.append(total)
    own_r = jnp.concatenate(pieces, axis=0)

    near_blocks = [(0, 0), (1, 0), (3, 0), (0, 1), (0, 3), (2, 0), (0, 2)]
    middle_blocks = [(1, 1), (1, 3), (3, 1), (3, 3)]
    far_blocks = [(2, 1), (2, 3), (1, 2), (3, 2)]

    def place_of(dx, dy, half):
        if dx != 0 and dy != 0:
            return 9 if (dx, dy) == (2, 2) else 0 if 2 in (dx, dy) else 8
        if half == 0:
            return dx if dy == 0 else 7
        return 3 + dy if dx == 0 else 7

    class Gather:
        def __init__(self, index, buffer):
            self.index, self.buffer = index, buffer

        def send(self, dx, dy, half, ex, ey):
            block = self.buffer.at[at(x + dx, y + dy), half]
            place = place_of((dx - ex) % SIDE, (dy - ey) % SIDE, half)
            push(block, block, send_sem.at[4 + self.index], gather_sem.at[self.index, place], device(at(x + ex, y + ey)))

        def arrive(self, place, ref):
            await_bytes(ref, gather_sem.at[self.index, place])

        def start(self, value):
            buffer = self.buffer
            high, low = split(value)
            for half in (0, 1):
                here = slice(half * HALF, (half + 1) * HALF)
                if self.index < 3:
                    buffer[chip, half, 0] = high[here]
                    buffer[chip, half, 1] = low[here]
                else:
                    buffer[chip, half] = high[here]
            for d in (2, 1, 3):
                self.send(0, 0, 0, d, 0)
                self.send(0, 0, 1, 0, d)

        def start_rest(self):
            for d in (2, 1, 3):
                self.send(0, 0, 0, 0, d)
                self.send(0, 0, 1, d, 0)

        def forward(self):
            half_block = self.buffer.at[0, 0]
            for d in (1, 3, 2):
                self.arrive(d, half_block)
                for e in (2, 1, 3):
                    self.send(d, 0, 0, 0, e)
                self.arrive(3 + d, half_block)
                for e in (2, 1, 3):
                    self.send(0, d, 1, e, 0)

        def near(self):
            self.arrive(7, self.buffer.at[pl.ds(0, 3)])

        def middle(self):
            self.arrive(8, self.buffer.at[pl.ds(0, 4)])

        def far(self):
            self.arrive(0, self.buffer.at[pl.ds(0, 4)])

        def last(self):
            self.arrive(9, self.buffer.at[0])

    def multiply(buffer, planes, blocks):
        places = [at(x + dx, y + dy) for dx, dy in blocks]
        left = jnp.concatenate([buffer[i].reshape(planes * MINE, WIDE) for i in places], axis=1)
        right = jnp.concatenate([matrix[i].reshape(2 * WIDE, WIDE) for i in places], axis=1)
        return lax.dot_general(left, right, (((1,), (1,)), ((), ())), preferred_element_type=F32)

    def fold(total, planes):
        if planes == 2:
            total = total.reshape(2, 2, HALF, 2 * WIDE)
            total = (total[:, 0] + total[:, 1]).reshape(MINE, 2 * WIDE)
        return jnp.concatenate(
            [total[:, i * WIDE : i * WIDE + ROWS] + total[:, i * WIDE + ROWS : (i + 1) * WIDE] for i in (0, 1)],
            axis=1,
        )

    def whole(buffer, planes, origin):
        block = buffer[origin].astype(F32)
        if planes == 2:
            block = block[:, 0] + block[:, 1]
        return block.reshape(MINE, WIDE)

    def products(gather, planes, blocks, first_time):
        for dx, dy in blocks:
            origin = at(x + dx, y + dy)
            block = whole(gather.buffer, planes, origin)
            if first_time:
                residual[origin] = block
                terms = block * block
            else:
                terms = residual[origin] * block
            dots[origin] = terms[:, :ROWS] + terms[:, ROWS:]
        return multiply(gather.buffer, planes, blocks)

    def finish(gather, planes, first_time=False):
        gather.forward()
        gather.near()
        height = planes * MINE
        product[:height] = products(gather, planes, near_blocks, first_time)
        gather.middle()
        product[:height] = product[:height] + products(gather, planes, middle_blocks, first_time)
        gather.far()
        product[:height] = product[:height] + products(gather, planes, far_blocks, first_time)
        gather.last()
        total = product[:height] + products(gather, planes, [(2, 2)], first_time)
        return fold(total, planes), column_sum(jnp.sum(dots[...], axis=0))

    zero = jnp.zeros((MINE, WIDE), F32)

    gather = Gather(0, gather_b)
    gather.start(own_r)
    hear_z(0)
    tell_z(1)
    await_bytes(matrix.at[:, other], matrix_sem)
    gather.start_rest()
    own_w, norm = finish(gather, 2, True)
    initial = norm

    alpha = beta = None
    own_p = own_s = own_t = own_x = None
    for step, (buffer, planes) in enumerate(((gather_0, 2), (gather_1, 2), (gather_2, 1))):
        gather = Gather(step + 1, buffer)
        gather.start(own_w)
        if step > 0:
            before, before_planes = ((gather_0, 2), (gather_1, 2))[step - 1]

            def advance(origin, total, buffer=before, planes=before_planes, step=step, alpha=alpha, beta=old_beta):
                direction = whole(buffer, planes, origin)
                if step > 1:
                    direction = direction + beta * mapped_dir[origin]
                mapped_dir[origin] = direction
                block = residual[origin] - alpha * direction
                residual[origin] = block
                return total + block * block

            following = column_sum(lax.fori_loop(0, CHIPS, advance, zero))
            beta = following / norm
            norm = following
        gather.start_rest()
        own_u, overlap = finish(gather, planes)
        if step == 0:
            alpha = norm / overlap
            own_p, own_s, own_t = own_r, own_w, own_u
            own_x = alpha * own_p
        else:
            alpha = norm / (overlap - beta * norm / alpha)
            own_p = own_r + beta * own_p
            own_s = own_w + beta * own_s
            own_t = own_u + beta * own_t
            own_x = own_x + alpha * own_p
        old_beta = beta
        own_r = own_r - alpha * own_s
        own_w = own_w - alpha * own_t

    def last_advance(origin, total):
        direction = whole(gather_2, 1, origin) + beta * mapped_dir[origin]
        block = residual[origin] - alpha * direction
        return total + block * block

    following = column_sum(lax.fori_loop(0, CHIPS, last_advance, zero))
    beta = following / norm
    norm = following

    own_s = own_w + beta * own_s
    own_p = own_r + beta * own_p
    close = own_r - alpha * own_s
    lane = lax.broadcasted_iota(jnp.int32, (MINE, ROWS), 1)
    def lay_flat(columns):
        packed = jnp.zeros((MINE, ROWS), F32)
        for i, column in enumerate(columns):
            packed = jnp.where(lane == i, column, packed)
        return jnp.transpose(jnp.concatenate([packed, jnp.zeros_like(packed)], axis=0))[: len(columns)]

    sums[chip] = lay_flat([column_sum(t) for t in (own_r * own_w, close * close, close * own_s, own_s * own_s)])

    def tell_chip(n, _):
        push(sums.at[chip], sums.at[chip], send_sem.at[8], sums_sem, device(lax.rem(chip + n, CHIPS)))
        return 0

    lax.fori_loop(1, CHIPS, tell_chip, 0)
    hear_z(1)
    known = lay_flat([norm, beta, alpha, initial])
    used = lax.broadcasted_iota(jnp.int32, (1, ROWS), 1) < MINE
    norm, beta, alpha, initial = (jnp.where(used, known[i : i + 1], 1.0) for i in range(4))
    await_bytes(sums.at[pl.ds(0, CHIPS - 1)], sums_sem)
    gathered = jnp.where(used, jnp.sum(sums[...], axis=0), 1.0)
    overlap, close_close, close_s, s_s = (gathered[i : i + 1] for i in range(4))
    last = norm / jnp.where(used, overlap - beta * norm / alpha, 1.0)
    excess = last - alpha
    final = jnp.maximum(close_close - 2.0 * excess * close_s + excess * excess * s_s, 0.0)

    place = grp * 2 + core
    final = column_sum(jnp.where(used, final, 0.0))
    initial = column_sum(jnp.where(used, initial, 0.0))
    totals[place] = jnp.where(lax.broadcasted_iota(jnp.int32, (1, ROWS), 1) == 0, final, initial)

    def tell_group(n, _):
        there = lax.rem(place + n, 2 * groups)
        push(
            totals.at[place], totals.at[place], send_sem.at[10], totals_sem,
            (lax.div(there, 2), chip * 2 + lax.rem(there, 2)),
        )
        return 0

    lax.fori_loop(1, 2 * groups, tell_group, 0)
    last = jnp.transpose(jnp.broadcast_to(last, (ROWS, ROWS)))[:MINE, :1]
    own_x = own_x + last * own_p
    answer[core, 0] = own_x[:, :ROWS]
    answer[core, 1] = own_x[:, ROWS:]
    push(answer.at[core, other], answer.at[core, other], send_sem.at[9], answer_sem, partner)
    await_bytes(answer.at[other, core], answer_sem)
    merged[...] = jnp.transpose(jnp.concatenate([answer[0, core], answer[1, core]], axis=0))

    await_bytes(partner_part, send_sem.at[0])
    await_bytes(matrix.at[:, 0], send_sem.at[1])
    await_bytes(first.at[:, pl.ds(0, 3)], send_sem.at[2])
    await_bytes(second.at[:, 0, pl.ds(0, 3)], send_sem.at[3])
    for i, buffer in enumerate((gather_b, gather_0, gather_1, gather_2)):
        await_bytes(buffer.at[pl.ds(0, CHIPS - 1)], send_sem.at[4 + i])
    await_bytes(sums.at[pl.ds(0, CHIPS - 1)], send_sem.at[8])
    await_bytes(answer.at[0, 0], send_sem.at[9])
    await_bytes(totals.at[pl.ds(0, 2 * groups - 1)], send_sem.at[10])
    await_bytes(totals.at[pl.ds(0, 2 * groups - 1)], totals_sem)
    over_all = jnp.sum(totals[...], axis=0)
    ratio[...] = jnp.sqrt(over_all[:, 0:1] / over_all[:, 1:2]) + jnp.zeros((1, ROWS), F32)


def local(expert_grams, expert_weights):
    groups = lax.axis_size("grp")
    hbm = pl.BlockSpec(memory_space=pltpu.HBM)
    vmem = pl.BlockSpec(memory_space=pltpu.VMEM)
    dma = pltpu.SemaphoreType.DMA
    merged, ratio = pl.pallas_call(
        kernel,
        out_shape=(jax.ShapeDtypeStruct((ROWS, COLS), F32), jax.ShapeDtypeStruct((1, ROWS), F32)),
        in_specs=[hbm, hbm],
        out_specs=(vmem, vmem),
        scratch_shapes=[
            pltpu.VMEM((CHIPS, EXPERTS, ROWS, WIDE), F32),
            pltpu.VMEM((CHIPS, 2, 2, ROWS, WIDE), BF16),
            pltpu.VMEM((EXPERTS, ROWS, COLS), BF16),
            pltpu.VMEM((COLS, 2 * EXPERTS * ROWS), BF16),
            pltpu.VMEM((CHIPS, 2, MINE, WIDE), F32),
            pltpu.VMEM((CHIPS, MINE, WIDE), F32),
            pltpu.VMEM((2, SIDE, SIDE, HALF, WIDE), F32),
            pltpu.VMEM((2, 2, SIDE, HALF, WIDE), F32),
            pltpu.VMEM((CHIPS, MINE, WIDE), F32),
            pltpu.VMEM((CHIPS, 2, 2, HALF, WIDE), BF16),
            pltpu.VMEM((CHIPS, 2, 2, HALF, WIDE), BF16),
            pltpu.VMEM((CHIPS, 2, 2, HALF, WIDE), BF16),
            pltpu.VMEM((CHIPS, 2, HALF, WIDE), BF16),
            pltpu.VMEM((CHIPS, MINE, WIDE), F32),
            pltpu.VMEM((CHIPS, MINE, WIDE), F32),
            pltpu.VMEM((CHIPS, MINE, ROWS), F32),
            pltpu.VMEM((2 * MINE, 2 * WIDE), F32),
            pltpu.VMEM((CHIPS, 4, ROWS), F32),
            pltpu.VMEM((2 * groups, 1, ROWS), F32),
            pltpu.VMEM((2, 2, MINE, ROWS), F32),
            dma((CHIPS // GROUP,)),
            dma((CHIPS // GROUP,)),
            dma,
            dma((2, SIDE)),
            dma((2,)),
            dma((4, 10)),
            dma,
            dma,
            dma,
            dma((11,)),
            dma((1,)),
            pltpu.SemaphoreType.REGULAR((2,)),
        ],
        compiler_params=pltpu.CompilerParams(
            collective_id=0, has_side_effects=True, vmem_limit_bytes=55040 * 1024
        ),
        name="merge",
    )(expert_grams, expert_weights)
    return merged, ratio[0, 0]


def solution(mesh):
    placed = (P(None, "row", None), P(None, "row", "grp"))
    return jax.shard_map(
        local, mesh=mesh, in_specs=placed, out_specs=(P("row", "grp"), P()), check_vma=False
    )
```

```python
import jax
import jax.numpy as jnp
from jax import lax
from jax.experimental import pallas as pl
from jax.experimental.pallas import tpu as pltpu
from jax.sharding import PartitionSpec as P

MESH = pl.DeviceIdType.MESH
F32, BF16 = jnp.float32, jnp.bfloat16
EXPERTS, ROWS, COLS = 4, 128, 128
CHIPS, SIDE, WIDE, MINE, HALF = 16, 4, 256, 64, 32
GROUP, BEFORE = 2, 0


def split(x):
    high = x.astype(BF16)
    return high, (x - high.astype(F32)).astype(BF16)


def column_sum(x):
    return jnp.sum(x, axis=1, keepdims=True)


def kernel(
    grams, weights, merged, ratio,
    panel, matrix, weights_in, weights_t, partial, partner_part, first, second, outgoing,
    gather_b, gather_0, gather_1, gather_2, residual, mapped_dir, dots, product,
    sums, totals, answer,
    panel_sem, partner_sem, matrix_sem, first_sem, second_sem, gather_sem, sums_sem, totals_sem, answer_sem,
    send_sem, local_sem, token_sem, turn_sem,
):
    grp, row = lax.axis_index("grp"), lax.axis_index("row")
    core, chip = lax.rem(row, 2), lax.div(row, 2)
    x, y = lax.div(chip, SIDE), lax.rem(chip, SIDE)
    other = 1 - core

    def at(cx, cy):
        return lax.rem(cx, SIDE) * SIDE + lax.rem(cy, SIDE)

    def device(target):
        return (grp, target * 2 + core)

    partner = (grp, chip * 2 + other)

    def push(src, dst, sent, arrived, to):
        pltpu.make_async_remote_copy(src, dst, sent, arrived, device_id=to, device_id_type=MESH).start()

    def await_bytes(ref, sem):
        pltpu.make_async_copy(ref, ref, sem).wait()

    groups = lax.axis_size("grp")
    barrier = pltpu.get_barrier_semaphore()
    along_z = [(lax.rem(grp + d, groups), row) for d in (2, groups - 2, 1, groups - 1)]
    lines = [device(at(x + d, y)) for d in (2, 1, 3)] + [device(at(x, y + d)) for d in (2, 1, 3)]
    order = [(2, 2), (1, 2), (3, 2), (2, 1), (2, 3), (1, 1), (3, 1), (1, 3), (3, 3)]
    order += [(0, 2), (2, 0), (0, 1), (1, 0), (0, 3), (3, 0), (0, 0)]
    targets = [at(x + dx, y + dy) for dx, dy in order]

    def panel_copy(n):
        columns = pl.ds(pl.multiple_of(targets[n] * WIDE, WIDE), WIDE)
        return pltpu.make_async_copy(grams.at[:, :, columns], panel.at[n], panel_sem.at[n // GROUP])

    weights_copy = pltpu.make_async_copy(weights, weights_in, local_sem.at[0])
    weights_copy.start()
    for n in range(GROUP):
        panel_copy(n).start()
    for there in (*along_z, *lines, partner):
        pl.semaphore_signal(barrier, 1, device_id=there, device_id_type=MESH)
    for n in range(GROUP, CHIPS):
        panel_copy(n).start()

    def tell_z(i):
        for there in along_z:
            pl.semaphore_signal(token_sem.at[i], 1, device_id=there, device_id_type=MESH)

    def hear_z(i):
        pl.semaphore_wait(token_sem.at[i], len(along_z))

    weights_copy.wait()
    turned = jnp.transpose(weights_in[...].reshape(EXPERTS * ROWS, COLS).astype(F32)).astype(BF16)
    weights_t[:, : EXPERTS * ROWS] = turned
    weights_t[:, EXPERTS * ROWS :] = turned

    def compute_panel(n):
        target = targets[n]
        high, low = split(panel[n].reshape(EXPERTS * ROWS, WIDE))
        product = jnp.dot(weights_t[...], jnp.concatenate([high, low], axis=0), preferred_element_type=F32)
        partial[target] = product.reshape(2, MINE, WIDE)
        system = (panel[n, 0] + panel[n, 1]) + (panel[n, 2] + panel[n, 3])
        if order[n] == (0, 0):
            below = lax.broadcasted_iota(jnp.int32, (ROWS, WIDE), 0) + core * ROWS
            system = system + (below == lax.broadcasted_iota(jnp.int32, (ROWS, WIDE), 1)).astype(F32)
        system_high, system_low = split(system)
        matrix[target, core, 0] = system_high
        matrix[target, core, 1] = system_low

    def swap_panel(n):
        target = targets[n]
        push(partial.at[target, other], partner_part.at[target], send_sem.at[0], partner_sem.at[n // GROUP], partner)

    def forward_panel(n):
        (dx, dy), target = order[n], targets[n]
        if n % GROUP == 0:
            await_bytes(partner_part.at[pl.ds(0, GROUP)], partner_sem.at[n // GROUP])
        outgoing[target] = partial[target, core] + partner_part[target]
        if dx != 0:
            push(
                outgoing.at[target, pl.ds(0, HALF)], first.at[0, x, lax.rem(y + dy, SIDE)],
                send_sem.at[2], first_sem.at[0, lax.rem(y + dy, SIDE)], device(at(x + dx, y)),
            )
        if dy != 0:
            push(
                outgoing.at[target, pl.ds(HALF, HALF)], first.at[1, y, lax.rem(x + dx, SIDE)],
                send_sem.at[2], first_sem.at[1, lax.rem(x + dx, SIDE)], device(at(x, y + dy)),
            )

    def compute_group(group):
        await_bytes(panel.at[pl.ds(0, GROUP)], panel_sem.at[group[0] // GROUP])
        for n in group:
            compute_panel(n)

    groups_of_panels = [range(i, i + GROUP) for i in range(0, CHIPS, GROUP)]
    for i, group in enumerate(groups_of_panels):
        compute_group(group)
        if i == BEFORE:
            pl.semaphore_wait(barrier, len(along_z) + len(lines) + 1)
            for earlier in groups_of_panels[:BEFORE]:
                for n in earlier:
                    swap_panel(n)
        if i >= BEFORE:
            for n in group:
                swap_panel(n)
        if i > BEFORE:
            for n in groups_of_panels[i - BEFORE - 1]:
                forward_panel(n)
    for group in groups_of_panels[len(groups_of_panels) - BEFORE - 1 :]:
        for n in group:
            forward_panel(n)

    def first_sum(half, k):
        line, along = (x, y) if half == 0 else (y, x)
        place = lax.rem(along + k, SIDE)
        target = at(x, place) if half == 0 else at(place, y)
        total = outgoing[target, pl.ds(half * HALF, HALF)]
        await_bytes(first.at[half, pl.ds(0, SIDE - 1), 0], first_sem.at[half, place])
        for j in (1, 3, 2):
            total = total + first[half, lax.rem(line + j, SIDE), place]
        return total, target

    tell_z(0)

    for k in (2, 1, 3):
        for half in (0, 1):
            along = y if half == 0 else x
            total, target = first_sum(half, k)
            second[half, 0, k] = total
            push(
                second.at[half, 0, k], second.at[half, 1, along],
                send_sem.at[3], second_sem.at[half], device(target),
            )
    def send_matrix(target, _):
        push(matrix.at[target, core], matrix.at[target, core], send_sem.at[1], matrix_sem, partner)
        return 0

    lax.fori_loop(0, CHIPS, send_matrix, 0)

    pieces = []
    for half in (0, 1):
        along = y if half == 0 else x
        total, _ = first_sum(half, 0)
        await_bytes(second.at[half, 1, pl.ds(0, SIDE - 1)], second_sem.at[half])
        for j in (1, 3, 2):
            total = total + second[half, 1, lax.rem(along + j, SIDE)]
        pieces.append(total)
    own_r = jnp.concatenate(pieces, axis=0)

    near_blocks = [(0, 0), (1, 0), (3, 0), (0, 1), (0, 3), (2, 0), (0, 2)]
    middle_blocks = [(1, 1), (1, 3), (3, 1), (3, 3)]
    far_blocks = [(2, 1), (2, 3), (1, 2), (3, 2)]

    def place_of(dx, dy, half):
        if dx != 0 and dy != 0:
            return 9 if (dx, dy) == (2, 2) else 0 if 2 in (dx, dy) else 8
        if half == 0:
            return dx if dy == 0 else 7
        return 3 + dy if dx == 0 else 7

    class Gather:
        def __init__(self, index, buffer):
            self.index, self.buffer = index, buffer

        def send(self, dx, dy, half, ex, ey):
            block = self.buffer.at[at(x + dx, y + dy), half]
            place = place_of((dx - ex) % SIDE, (dy - ey) % SIDE, half)
            push(block, block, send_sem.at[4 + self.index], gather_sem.at[self.index, place], device(at(x + ex, y + ey)))

        def arrive(self, place, ref):
            await_bytes(ref, gather_sem.at[self.index, place])

        def start(self, value):
            buffer = self.buffer
            high, low = split(value)
            for half in (0, 1):
                here = slice(half * HALF, (half + 1) * HALF)
                if self.index < 3:
                    buffer[chip, half, 0] = high[here]
                    buffer[chip, half, 1] = low[here]
                else:
                    buffer[chip, half] = high[here]
            if self.index > 0:

                @pl.when(core == 1)
                def _():
                    pl.semaphore_wait(turn_sem, 1)

            for d in (2, 1, 3):
                self.send(0, 0, 0, d, 0)
                self.send(0, 0, 1, 0, d)

        def start_rest(self):
            for d in (2, 1, 3):
                self.send(0, 0, 0, 0, d)
                self.send(0, 0, 1, d, 0)

        def forward(self):
            half_block = self.buffer.at[0, 0]
            for d in (1, 3, 2):
                self.arrive(d, half_block)
                for e in (2, 1, 3):
                    self.send(d, 0, 0, 0, e)
                self.arrive(3 + d, half_block)
                for e in (2, 1, 3):
                    self.send(0, d, 1, e, 0)

        def pass_turn(self):
            @pl.when(core == 0)
            def _():
                pl.semaphore_signal(turn_sem, 1, device_id=partner, device_id_type=MESH)

        def near(self):
            self.arrive(7, self.buffer.at[pl.ds(0, 3)])

        def middle(self):
            self.arrive(8, self.buffer.at[pl.ds(0, 4)])

        def far(self):
            self.arrive(0, self.buffer.at[pl.ds(0, 4)])

        def last(self):
            self.arrive(9, self.buffer.at[0])

    def multiply(buffer, planes, blocks):
        places = [at(x + dx, y + dy) for dx, dy in blocks]
        left = jnp.concatenate([buffer[i].reshape(planes * MINE, WIDE) for i in places], axis=1)
        right = jnp.concatenate([matrix[i].reshape(2 * WIDE, WIDE) for i in places], axis=1)
        return lax.dot_general(left, right, (((1,), (1,)), ((), ())), preferred_element_type=F32)

    def fold(total, planes):
        if planes == 2:
            total = total.reshape(2, 2, HALF, 2 * WIDE)
            total = (total[:, 0] + total[:, 1]).reshape(MINE, 2 * WIDE)
        return jnp.concatenate(
            [total[:, i * WIDE : i * WIDE + ROWS] + total[:, i * WIDE + ROWS : (i + 1) * WIDE] for i in (0, 1)],
            axis=1,
        )

    def whole(buffer, planes, origin):
        block = buffer[origin].astype(F32)
        if planes == 2:
            block = block[:, 0] + block[:, 1]
        return block.reshape(MINE, WIDE)

    def products(gather, planes, blocks, first_time):
        for dx, dy in blocks:
            origin = at(x + dx, y + dy)
            block = whole(gather.buffer, planes, origin)
            if first_time:
                residual[origin] = block
                terms = block * block
            else:
                terms = residual[origin] * block
            dots[origin] = terms[:, :ROWS] + terms[:, ROWS:]
        return multiply(gather.buffer, planes, blocks)

    def finish(gather, planes, first_time=False):
        gather.forward()
        gather.near()
        height = planes * MINE
        product[:height] = products(gather, planes, near_blocks, first_time)
        gather.middle()
        product[:height] = product[:height] + products(gather, planes, middle_blocks, first_time)
        gather.far()
        if gather.index < 3:
            gather.pass_turn()
        product[:height] = product[:height] + products(gather, planes, far_blocks, first_time)
        gather.last()
        total = product[:height] + products(gather, planes, [(2, 2)], first_time)
        return fold(total, planes), column_sum(jnp.sum(dots[...], axis=0))

    zero = jnp.zeros((MINE, WIDE), F32)

    gather = Gather(0, gather_b)
    gather.start(own_r)
    hear_z(0)
    tell_z(1)
    await_bytes(matrix.at[:, other], matrix_sem)
    gather.start_rest()
    own_w, norm = finish(gather, 2, True)
    initial = norm

    alpha = beta = None
    own_p = own_s = own_t = own_x = None
    for step, (buffer, planes) in enumerate(((gather_0, 2), (gather_1, 2), (gather_2, 1))):
        gather = Gather(step + 1, buffer)
        gather.start(own_w)
        gather.start_rest()
        if step > 0:
            before, before_planes = ((gather_0, 2), (gather_1, 2))[step - 1]

            def advance(origin, total, buffer=before, planes=before_planes, step=step, alpha=alpha, beta=old_beta):
                direction = whole(buffer, planes, origin)
                if step > 1:
                    direction = direction + beta * mapped_dir[origin]
                mapped_dir[origin] = direction
                block = residual[origin] - alpha * direction
                residual[origin] = block
                return total + block * block

            following = column_sum(lax.fori_loop(0, CHIPS, advance, zero))
            beta = following / norm
            norm = following
        own_u, overlap = finish(gather, planes)
        if step == 0:
            alpha = norm / overlap
            own_p, own_s, own_t = own_r, own_w, own_u
            own_x = alpha * own_p
        else:
            alpha = norm / (overlap - beta * norm / alpha)
            own_p = own_r + beta * own_p
            own_s = own_w + beta * own_s
            own_t = own_u + beta * own_t
            own_x = own_x + alpha * own_p
        old_beta = beta
        own_r = own_r - alpha * own_s
        own_w = own_w - alpha * own_t

    alpha_beta = alpha * beta
    close = own_r - alpha * own_w - alpha_beta * own_s
    lane = lax.broadcasted_iota(jnp.int32, (MINE, ROWS), 1)

    def pack(columns):
        packed = jnp.zeros((MINE, ROWS), F32)
        for i, column in enumerate(columns):
            packed = jnp.where(lane == i, column, packed)
        return packed

    def lay_flat(left, right):
        return jnp.transpose(jnp.concatenate([pack(left), pack(right)], axis=0))

    sums[chip] = lay_flat(
        [column_sum(t) for t in (own_r * own_w, close * close, close * own_w, close * own_s)],
        [column_sum(t) for t in (own_w * own_w, own_w * own_s, own_s * own_s)],
    )[:4]

    def tell_chip(n, _):
        push(sums.at[chip], sums.at[chip], send_sem.at[8], sums_sem, device(lax.rem(chip + n, CHIPS)))
        return 0

    lax.fori_loop(1, CHIPS, tell_chip, 0)
    def last_advance(origin, total):
        direction = whole(gather_2, 1, origin) + beta * mapped_dir[origin]
        block = residual[origin] - alpha * direction
        return total + block * block

    following = column_sum(lax.fori_loop(0, CHIPS, last_advance, zero))
    beta = following / norm
    norm = following
    own_p = own_r + beta * own_p
    hear_z(1)
    known = lay_flat([norm, beta, alpha, initial, alpha_beta], [])
    used = lax.broadcasted_iota(jnp.int32, (1, ROWS), 1) < MINE
    norm, beta, alpha, initial, alpha_beta = (jnp.where(used, known[i : i + 1], 1.0) for i in range(5))
    await_bytes(sums.at[pl.ds(0, CHIPS - 1)], sums_sem)
    gathered = jnp.sum(sums[...], axis=0)
    gathered = jnp.concatenate([gathered, pltpu.roll(gathered, MINE, 1)], axis=0)
    overlap, c_c, c_w, c_s, w_w, w_s, s_s = (jnp.where(used, gathered[i : i + 1], 1.0) for i in range(7))
    last = norm / jnp.where(used, overlap - beta * norm / alpha, 1.0)
    more_w, more_s = last - alpha, last * beta - alpha_beta
    final = c_c - 2.0 * (more_w * c_w + more_s * c_s) + more_w * more_w * w_w
    final = jnp.maximum(final + more_s * (2.0 * more_w * w_s + more_s * s_s), 0.0)

    place = grp * 2 + core
    final = column_sum(jnp.where(used, final, 0.0))
    initial = column_sum(jnp.where(used, initial, 0.0))
    totals[place] = jnp.where(lax.broadcasted_iota(jnp.int32, (1, ROWS), 1) == 0, final, initial)

    def tell_group(n, _):
        there = lax.rem(place + n, 2 * groups)
        push(
            totals.at[place], totals.at[place], send_sem.at[10], totals_sem,
            (lax.div(there, 2), chip * 2 + lax.rem(there, 2)),
        )
        return 0

    lax.fori_loop(1, 2 * groups, tell_group, 0)
    last = jnp.transpose(jnp.broadcast_to(last, (ROWS, ROWS)))[:MINE, :1]
    own_x = own_x + last * own_p
    answer[core, 0] = own_x[:, :ROWS]
    answer[core, 1] = own_x[:, ROWS:]
    push(answer.at[core, other], answer.at[core, other], send_sem.at[9], answer_sem, partner)
    await_bytes(answer.at[other, core], answer_sem)
    merged[...] = jnp.transpose(jnp.concatenate([answer[0, core], answer[1, core]], axis=0))

    await_bytes(partner_part, send_sem.at[0])
    await_bytes(matrix.at[:, 0], send_sem.at[1])
    await_bytes(first.at[:, pl.ds(0, 3)], send_sem.at[2])
    await_bytes(second.at[:, 0, pl.ds(0, 3)], send_sem.at[3])
    for i, buffer in enumerate((gather_b, gather_0, gather_1, gather_2)):
        await_bytes(buffer.at[pl.ds(0, CHIPS - 1)], send_sem.at[4 + i])
    await_bytes(sums.at[pl.ds(0, CHIPS - 1)], send_sem.at[8])
    await_bytes(answer.at[0, 0], send_sem.at[9])
    await_bytes(totals.at[pl.ds(0, 2 * groups - 1)], send_sem.at[10])
    await_bytes(totals.at[pl.ds(0, 2 * groups - 1)], totals_sem)
    over_all = jnp.sum(totals[...], axis=0)
    ratio[...] = jnp.sqrt(over_all[:, 0:1] / over_all[:, 1:2]) + jnp.zeros((1, ROWS), F32)


def local(expert_grams, expert_weights):
    groups = lax.axis_size("grp")
    hbm = pl.BlockSpec(memory_space=pltpu.HBM)
    vmem = pl.BlockSpec(memory_space=pltpu.VMEM)
    dma = pltpu.SemaphoreType.DMA
    merged, ratio = pl.pallas_call(
        kernel,
        out_shape=(jax.ShapeDtypeStruct((ROWS, COLS), F32), jax.ShapeDtypeStruct((1, ROWS), F32)),
        in_specs=[hbm, hbm],
        out_specs=(vmem, vmem),
        scratch_shapes=[
            pltpu.VMEM((CHIPS, EXPERTS, ROWS, WIDE), F32),
            pltpu.VMEM((CHIPS, 2, 2, ROWS, WIDE), BF16),
            pltpu.VMEM((EXPERTS, ROWS, COLS), BF16),
            pltpu.VMEM((COLS, 2 * EXPERTS * ROWS), BF16),
            pltpu.VMEM((CHIPS, 2, MINE, WIDE), F32),
            pltpu.VMEM((CHIPS, MINE, WIDE), F32),
            pltpu.VMEM((2, SIDE, SIDE, HALF, WIDE), F32),
            pltpu.VMEM((2, 2, SIDE, HALF, WIDE), F32),
            pltpu.VMEM((CHIPS, MINE, WIDE), F32),
            pltpu.VMEM((CHIPS, 2, 2, HALF, WIDE), BF16),
            pltpu.VMEM((CHIPS, 2, 2, HALF, WIDE), BF16),
            pltpu.VMEM((CHIPS, 2, 2, HALF, WIDE), BF16),
            pltpu.VMEM((CHIPS, 2, HALF, WIDE), BF16),
            pltpu.VMEM((CHIPS, MINE, WIDE), F32),
            pltpu.VMEM((CHIPS, MINE, WIDE), F32),
            pltpu.VMEM((CHIPS, MINE, ROWS), F32),
            pltpu.VMEM((2 * MINE, 2 * WIDE), F32),
            pltpu.VMEM((CHIPS, 4, ROWS), F32),
            pltpu.VMEM((2 * groups, 1, ROWS), F32),
            pltpu.VMEM((2, 2, MINE, ROWS), F32),
            dma((CHIPS // GROUP,)),
            dma((CHIPS // GROUP,)),
            dma,
            dma((2, SIDE)),
            dma((2,)),
            dma((4, 10)),
            dma,
            dma,
            dma,
            dma((11,)),
            dma((1,)),
            pltpu.SemaphoreType.REGULAR((2,)),
            pltpu.SemaphoreType.REGULAR,
        ],
        compiler_params=pltpu.CompilerParams(
            collective_id=0, has_side_effects=True, vmem_limit_bytes=55040 * 1024
        ),
        name="merge",
    )(expert_grams, expert_weights)
    return merged, ratio[0, 0]


def solution(mesh):
    placed = (P(None, "row", None), P(None, "row", "grp"))
    return jax.shard_map(
        local, mesh=mesh, in_specs=placed, out_specs=(P("row", "grp"), P()), check_vma=False
    )
```

```python
import jax
import jax.numpy as jnp
from jax import lax
from jax.experimental import pallas as pl
from jax.experimental.pallas import tpu as pltpu
from jax.sharding import PartitionSpec as P

MESH = pl.DeviceIdType.MESH
F32, BF16 = jnp.float32, jnp.bfloat16
EXPERTS, ROWS, COLS = 4, 128, 128
CHIPS, SIDE, WIDE, MINE, HALF = 16, 4, 256, 64, 32
GROUP, BEFORE = 2, 0


def split(x):
    high = x.astype(BF16)
    return high, (x - high.astype(F32)).astype(BF16)


def column_sum(x):
    return jnp.sum(x, axis=1, keepdims=True)


def kernel(
    grams, weights, merged, ratio,
    panel, matrix, weights_in, weights_t, partial, partner_part, first, second, outgoing,
    gather_b, gather_0, gather_1, gather_2, residual, mapped_dir, dots, product,
    sums, totals, answer,
    panel_sem, partner_sem, matrix_sem, first_sem, second_sem, gather_sem, sums_sem, totals_sem, answer_sem,
    send_sem, local_sem, token_sem, turn_sem,
):
    grp, row = lax.axis_index("grp"), lax.axis_index("row")
    core, chip = lax.rem(row, 2), lax.div(row, 2)
    x, y = lax.div(chip, SIDE), lax.rem(chip, SIDE)
    other = 1 - core

    def at(cx, cy):
        return lax.rem(cx, SIDE) * SIDE + lax.rem(cy, SIDE)

    def device(target):
        return (grp, target * 2 + core)

    partner = (grp, chip * 2 + other)

    def push(src, dst, sent, arrived, to):
        pltpu.make_async_remote_copy(src, dst, sent, arrived, device_id=to, device_id_type=MESH).start()

    def await_bytes(ref, sem):
        pltpu.make_async_copy(ref, ref, sem).wait()

    groups = lax.axis_size("grp")
    barrier = pltpu.get_barrier_semaphore()
    along_z = [(lax.rem(grp + d, groups), row) for d in (2, groups - 2, 1, groups - 1)]
    lines = [device(at(x + d, y)) for d in (2, 1, 3)] + [device(at(x, y + d)) for d in (2, 1, 3)]
    order = [(2, 2), (1, 2), (3, 2), (2, 1), (2, 3), (1, 1), (3, 1), (1, 3), (3, 3)]
    order += [(0, 2), (2, 0), (0, 1), (1, 0), (0, 3), (3, 0), (0, 0)]
    targets = [at(x + dx, y + dy) for dx, dy in order]

    def panel_copy(n):
        columns = pl.ds(pl.multiple_of(targets[n] * WIDE, WIDE), WIDE)
        return pltpu.make_async_copy(grams.at[:, :, columns], panel.at[n], panel_sem.at[n // GROUP])

    weights_copy = pltpu.make_async_copy(weights, weights_in, local_sem.at[0])
    weights_copy.start()
    for n in range(GROUP):
        panel_copy(n).start()
    for there in (*along_z, *lines, partner):
        pl.semaphore_signal(barrier, 1, device_id=there, device_id_type=MESH)
    for n in range(GROUP, CHIPS):
        panel_copy(n).start()

    def tell_z(i):
        for there in along_z:
            pl.semaphore_signal(token_sem.at[i], 1, device_id=there, device_id_type=MESH)

    def hear_z(i):
        pl.semaphore_wait(token_sem.at[i], len(along_z))

    weights_copy.wait()
    turned = jnp.transpose(weights_in[...].reshape(EXPERTS * ROWS, COLS).astype(F32)).astype(BF16)
    weights_t[:, : EXPERTS * ROWS] = turned
    weights_t[:, EXPERTS * ROWS :] = turned

    def compute_panel(n):
        target = targets[n]
        high, low = split(panel[n].reshape(EXPERTS * ROWS, WIDE))
        product = jnp.dot(weights_t[...], jnp.concatenate([high, low], axis=0), preferred_element_type=F32)
        partial[target] = product.reshape(2, MINE, WIDE)
        system = (panel[n, 0] + panel[n, 1]) + (panel[n, 2] + panel[n, 3])
        if order[n] == (0, 0):
            below = lax.broadcasted_iota(jnp.int32, (ROWS, WIDE), 0) + core * ROWS
            system = system + (below == lax.broadcasted_iota(jnp.int32, (ROWS, WIDE), 1)).astype(F32)
        system_high, system_low = split(system)
        matrix[target, core, 0] = system_high
        matrix[target, core, 1] = system_low

    def swap_panel(n):
        target = targets[n]
        push(partial.at[target, other], partner_part.at[target], send_sem.at[0], partner_sem.at[n // GROUP], partner)

    def forward_panel(n):
        (dx, dy), target = order[n], targets[n]
        if n % GROUP == 0:
            await_bytes(partner_part.at[pl.ds(0, GROUP)], partner_sem.at[n // GROUP])
        outgoing[target] = partial[target, core] + partner_part[target]
        if dx != 0:
            push(
                outgoing.at[target, pl.ds(0, HALF)], first.at[0, x, lax.rem(y + dy, SIDE)],
                send_sem.at[2], first_sem.at[0, lax.rem(y + dy, SIDE)], device(at(x + dx, y)),
            )
        if dy != 0:
            push(
                outgoing.at[target, pl.ds(HALF, HALF)], first.at[1, y, lax.rem(x + dx, SIDE)],
                send_sem.at[2], first_sem.at[1, lax.rem(x + dx, SIDE)], device(at(x, y + dy)),
            )

    def compute_group(group):
        await_bytes(panel.at[pl.ds(0, GROUP)], panel_sem.at[group[0] // GROUP])
        for n in group:
            compute_panel(n)

    groups_of_panels = [range(i, i + GROUP) for i in range(0, CHIPS, GROUP)]
    for i, group in enumerate(groups_of_panels):
        compute_group(group)
        if i == BEFORE:
            pl.semaphore_wait(barrier, len(along_z) + len(lines) + 1)
            for earlier in groups_of_panels[:BEFORE]:
                for n in earlier:
                    swap_panel(n)
        if i >= BEFORE:
            for n in group:
                swap_panel(n)
        if i > BEFORE:
            for n in groups_of_panels[i - BEFORE - 1]:
                forward_panel(n)
    for group in groups_of_panels[len(groups_of_panels) - BEFORE - 1 :]:
        for n in group:
            forward_panel(n)

    def first_sum(half, k):
        line, along = (x, y) if half == 0 else (y, x)
        place = lax.rem(along + k, SIDE)
        target = at(x, place) if half == 0 else at(place, y)
        total = outgoing[target, pl.ds(half * HALF, HALF)]
        await_bytes(first.at[half, pl.ds(0, SIDE - 1), 0], first_sem.at[half, place])
        for j in (1, 3, 2):
            total = total + first[half, lax.rem(line + j, SIDE), place]
        return total, target

    tell_z(0)

    for k in (2, 1, 3):
        for half in (0, 1):
            along = y if half == 0 else x
            total, target = first_sum(half, k)
            second[half, 0, k] = total
            push(
                second.at[half, 0, k], second.at[half, 1, along],
                send_sem.at[3], second_sem.at[half], device(target),
            )
    def send_matrix(target, _):
        push(matrix.at[target, core], matrix.at[target, core], send_sem.at[1], matrix_sem, partner)
        return 0

    lax.fori_loop(0, CHIPS, send_matrix, 0)


    near_blocks = [(0, 0), (1, 0), (3, 0), (0, 1), (0, 3), (2, 0), (0, 2)]
    middle_blocks = [(1, 1), (1, 3), (3, 1), (3, 3)]
    far_blocks = [(2, 1), (2, 3), (1, 2), (3, 2)]

    def place_of(dx, dy, half):
        if dx != 0 and dy != 0:
            return 9 if (dx, dy) == (2, 2) else 0 if 2 in (dx, dy) else 8
        if half == 0:
            return dx if dy == 0 else 7
        return 3 + dy if dx == 0 else 7

    class Gather:
        def __init__(self, index, buffer):
            self.index, self.buffer = index, buffer

        def send(self, dx, dy, half, ex, ey):
            block = self.buffer.at[at(x + dx, y + dy), half]
            place = place_of((dx - ex) % SIDE, (dy - ey) % SIDE, half)
            push(block, block, send_sem.at[4 + self.index], gather_sem.at[self.index, place], device(at(x + ex, y + ey)))

        def arrive(self, place, ref):
            await_bytes(ref, gather_sem.at[self.index, place])

        def start_half(self, half, value):
            self.buffer[chip, half, 0], self.buffer[chip, half, 1] = split(value)
            for d in (2, 1, 3):
                self.send(0, 0, half, *((d, 0) if half == 0 else (0, d)))

        def start(self, value):
            buffer = self.buffer
            high, low = split(value)
            for half in (0, 1):
                here = slice(half * HALF, (half + 1) * HALF)
                if self.index < 3:
                    buffer[chip, half, 0] = high[here]
                    buffer[chip, half, 1] = low[here]
                else:
                    buffer[chip, half] = high[here]
            if self.index > 0:

                @pl.when(core == 1)
                def _():
                    pl.semaphore_wait(turn_sem, 1)

            for d in (2, 1, 3):
                self.send(0, 0, 0, d, 0)
                self.send(0, 0, 1, 0, d)

        def start_rest(self):
            for d in (2, 1, 3):
                self.send(0, 0, 0, 0, d)
                self.send(0, 0, 1, d, 0)

        def forward(self):
            half_block = self.buffer.at[0, 0]
            for d in (1, 3, 2):
                self.arrive(d, half_block)
                for e in (2, 1, 3):
                    self.send(d, 0, 0, 0, e)
                self.arrive(3 + d, half_block)
                for e in (2, 1, 3):
                    self.send(0, d, 1, e, 0)

        def pass_turn(self):
            @pl.when(core == 0)
            def _():
                pl.semaphore_signal(turn_sem, 1, device_id=partner, device_id_type=MESH)

        def near(self):
            self.arrive(7, self.buffer.at[pl.ds(0, 3)])

        def middle(self):
            self.arrive(8, self.buffer.at[pl.ds(0, 4)])

        def far(self):
            self.arrive(0, self.buffer.at[pl.ds(0, 4)])

        def last(self):
            self.arrive(9, self.buffer.at[0])

    def multiply(buffer, planes, blocks):
        places = [at(x + dx, y + dy) for dx, dy in blocks]
        left = jnp.concatenate([buffer[i].reshape(planes * MINE, WIDE) for i in places], axis=1)
        right = jnp.concatenate([matrix[i].reshape(2 * WIDE, WIDE) for i in places], axis=1)
        return lax.dot_general(left, right, (((1,), (1,)), ((), ())), preferred_element_type=F32)

    def fold(total, planes):
        if planes == 2:
            total = total.reshape(2, 2, HALF, 2 * WIDE)
            total = (total[:, 0] + total[:, 1]).reshape(MINE, 2 * WIDE)
        return jnp.concatenate(
            [total[:, i * WIDE : i * WIDE + ROWS] + total[:, i * WIDE + ROWS : (i + 1) * WIDE] for i in (0, 1)],
            axis=1,
        )

    def whole(buffer, planes, origin):
        block = buffer[origin].astype(F32)
        if planes == 2:
            block = block[:, 0] + block[:, 1]
        return block.reshape(MINE, WIDE)

    def products(gather, planes, blocks, first_time):
        for dx, dy in blocks:
            origin = at(x + dx, y + dy)
            block = whole(gather.buffer, planes, origin)
            if first_time:
                residual[origin] = block
                terms = block * block
            else:
                terms = residual[origin] * block
            dots[origin] = terms[:, :ROWS] + terms[:, ROWS:]
        return multiply(gather.buffer, planes, blocks)

    def finish(gather, planes, first_time=False):
        gather.forward()
        gather.near()
        height = planes * MINE
        product[:height] = products(gather, planes, near_blocks, first_time)
        gather.middle()
        product[:height] = product[:height] + products(gather, planes, middle_blocks, first_time)
        gather.far()
        if gather.index < 3:
            gather.pass_turn()
        product[:height] = product[:height] + products(gather, planes, far_blocks, first_time)
        gather.last()
        total = product[:height] + products(gather, planes, [(2, 2)], first_time)
        return fold(total, planes), column_sum(jnp.sum(dots[...], axis=0))

    zero = jnp.zeros((MINE, WIDE), F32)

    gather = Gather(0, gather_b)
    pieces = []
    for half in (0, 1):
        along = y if half == 0 else x
        total, _ = first_sum(half, 0)
        await_bytes(second.at[half, 1, pl.ds(0, SIDE - 1)], second_sem.at[half])
        for j in (1, 3, 2):
            total = total + second[half, 1, lax.rem(along + j, SIDE)]
        pieces.append(total)
        gather.start_half(half, total)
    own_r = jnp.concatenate(pieces, axis=0)

    hear_z(0)
    tell_z(1)
    await_bytes(matrix.at[:, other], matrix_sem)
    gather.start_rest()
    own_w, norm = finish(gather, 2, True)
    initial = norm

    alpha = beta = None
    own_p = own_s = own_t = own_x = None
    for step, (buffer, planes) in enumerate(((gather_0, 2), (gather_1, 2), (gather_2, 1))):
        gather = Gather(step + 1, buffer)
        gather.start(own_w)
        gather.start_rest()
        if step > 0:
            before, before_planes = ((gather_0, 2), (gather_1, 2))[step - 1]

            def advance(origin, total, buffer=before, planes=before_planes, step=step, alpha=alpha, beta=old_beta):
                direction = whole(buffer, planes, origin)
                if step > 1:
                    direction = direction + beta * mapped_dir[origin]
                mapped_dir[origin] = direction
                block = residual[origin] - alpha * direction
                residual[origin] = block
                return total + block * block

            following = column_sum(lax.fori_loop(0, CHIPS, advance, zero))
            beta = following / norm
            norm = following
        own_u, overlap = finish(gather, planes)
        if step == 0:
            alpha = norm / overlap
            own_p, own_s, own_t = own_r, own_w, own_u
            own_x = alpha * own_p
        else:
            alpha = norm / (overlap - beta * norm / alpha)
            own_p = own_r + beta * own_p
            own_s = own_w + beta * own_s
            own_t = own_u + beta * own_t
            own_x = own_x + alpha * own_p
        old_beta = beta
        own_r = own_r - alpha * own_s
        own_w = own_w - alpha * own_t

    alpha_beta = alpha * beta
    close = own_r - alpha * own_w - alpha_beta * own_s
    lane = lax.broadcasted_iota(jnp.int32, (MINE, ROWS), 1)

    def pack(columns):
        packed = jnp.zeros((MINE, ROWS), F32)
        for i, column in enumerate(columns):
            packed = jnp.where(lane == i, column, packed)
        return packed

    def lay_flat(left, right):
        return jnp.transpose(jnp.concatenate([pack(left), pack(right)], axis=0))

    sums[chip] = lay_flat(
        [column_sum(t) for t in (own_r * own_w, close * close, close * own_w, close * own_s)],
        [column_sum(t) for t in (own_w * own_w, own_w * own_s, own_s * own_s)],
    )[:4]

    def tell_chip(n, _):
        push(sums.at[chip], sums.at[chip], send_sem.at[8], sums_sem, device(lax.rem(chip + n, CHIPS)))
        return 0

    lax.fori_loop(1, CHIPS, tell_chip, 0)
    def last_advance(origin, total):
        direction = whole(gather_2, 1, origin) + beta * mapped_dir[origin]
        block = residual[origin] - alpha * direction
        return total + block * block

    following = column_sum(lax.fori_loop(0, CHIPS, last_advance, zero))
    beta = following / norm
    norm = following
    own_p = own_r + beta * own_p
    hear_z(1)
    known = lay_flat([norm, beta, alpha, initial, alpha_beta], [])
    used = lax.broadcasted_iota(jnp.int32, (1, ROWS), 1) < MINE
    norm, beta, alpha, initial, alpha_beta = (jnp.where(used, known[i : i + 1], 1.0) for i in range(5))
    await_bytes(sums.at[pl.ds(0, CHIPS - 1)], sums_sem)
    gathered = jnp.sum(sums[...], axis=0)
    gathered = jnp.concatenate([gathered, pltpu.roll(gathered, MINE, 1)], axis=0)
    overlap, c_c, c_w, c_s, w_w, w_s, s_s = (jnp.where(used, gathered[i : i + 1], 1.0) for i in range(7))
    last = norm / jnp.where(used, overlap - beta * norm / alpha, 1.0)
    more_w, more_s = last - alpha, last * beta - alpha_beta
    final = c_c - 2.0 * (more_w * c_w + more_s * c_s) + more_w * more_w * w_w
    final = jnp.maximum(final + more_s * (2.0 * more_w * w_s + more_s * s_s), 0.0)

    place = grp * 2 + core
    final = column_sum(jnp.where(used, final, 0.0))
    initial = column_sum(jnp.where(used, initial, 0.0))
    totals[place] = jnp.where(lax.broadcasted_iota(jnp.int32, (1, ROWS), 1) == 0, final, initial)

    def tell_group(n, _):
        there = lax.rem(place + n, 2 * groups)
        push(
            totals.at[place], totals.at[place], send_sem.at[10], totals_sem,
            (lax.div(there, 2), chip * 2 + lax.rem(there, 2)),
        )
        return 0

    lax.fori_loop(1, 2 * groups, tell_group, 0)
    last = jnp.transpose(jnp.broadcast_to(last, (ROWS, ROWS)))[:MINE, :1]
    own_x = own_x + last * own_p
    answer[core, 0] = own_x[:, :ROWS]
    answer[core, 1] = own_x[:, ROWS:]
    push(answer.at[core, other], answer.at[core, other], send_sem.at[9], answer_sem, partner)
    await_bytes(answer.at[other, core], answer_sem)
    merged[...] = jnp.transpose(jnp.concatenate([answer[0, core], answer[1, core]], axis=0))

    await_bytes(partner_part, send_sem.at[0])
    await_bytes(matrix.at[:, 0], send_sem.at[1])
    await_bytes(first.at[:, pl.ds(0, 3)], send_sem.at[2])
    await_bytes(second.at[:, 0, pl.ds(0, 3)], send_sem.at[3])
    for i, buffer in enumerate((gather_b, gather_0, gather_1, gather_2)):
        await_bytes(buffer.at[pl.ds(0, CHIPS - 1)], send_sem.at[4 + i])
    await_bytes(sums.at[pl.ds(0, CHIPS - 1)], send_sem.at[8])
    await_bytes(answer.at[0, 0], send_sem.at[9])
    await_bytes(totals.at[pl.ds(0, 2 * groups - 1)], send_sem.at[10])
    await_bytes(totals.at[pl.ds(0, 2 * groups - 1)], totals_sem)
    over_all = jnp.sum(totals[...], axis=0)
    ratio[...] = jnp.sqrt(over_all[:, 0:1] / over_all[:, 1:2]) + jnp.zeros((1, ROWS), F32)


def local(expert_grams, expert_weights):
    groups = lax.axis_size("grp")
    hbm = pl.BlockSpec(memory_space=pltpu.HBM)
    vmem = pl.BlockSpec(memory_space=pltpu.VMEM)
    dma = pltpu.SemaphoreType.DMA
    merged, ratio = pl.pallas_call(
        kernel,
        out_shape=(jax.ShapeDtypeStruct((ROWS, COLS), F32), jax.ShapeDtypeStruct((1, ROWS), F32)),
        in_specs=[hbm, hbm],
        out_specs=(vmem, vmem),
        scratch_shapes=[
            pltpu.VMEM((CHIPS, EXPERTS, ROWS, WIDE), F32),
            pltpu.VMEM((CHIPS, 2, 2, ROWS, WIDE), BF16),
            pltpu.VMEM((EXPERTS, ROWS, COLS), BF16),
            pltpu.VMEM((COLS, 2 * EXPERTS * ROWS), BF16),
            pltpu.VMEM((CHIPS, 2, MINE, WIDE), F32),
            pltpu.VMEM((CHIPS, MINE, WIDE), F32),
            pltpu.VMEM((2, SIDE, SIDE, HALF, WIDE), F32),
            pltpu.VMEM((2, 2, SIDE, HALF, WIDE), F32),
            pltpu.VMEM((CHIPS, MINE, WIDE), F32),
            pltpu.VMEM((CHIPS, 2, 2, HALF, WIDE), BF16),
            pltpu.VMEM((CHIPS, 2, 2, HALF, WIDE), BF16),
            pltpu.VMEM((CHIPS, 2, 2, HALF, WIDE), BF16),
            pltpu.VMEM((CHIPS, 2, HALF, WIDE), BF16),
            pltpu.VMEM((CHIPS, MINE, WIDE), F32),
            pltpu.VMEM((CHIPS, MINE, WIDE), F32),
            pltpu.VMEM((CHIPS, MINE, ROWS), F32),
            pltpu.VMEM((2 * MINE, 2 * WIDE), F32),
            pltpu.VMEM((CHIPS, 4, ROWS), F32),
            pltpu.VMEM((2 * groups, 1, ROWS), F32),
            pltpu.VMEM((2, 2, MINE, ROWS), F32),
            dma((CHIPS // GROUP,)),
            dma((CHIPS // GROUP,)),
            dma,
            dma((2, SIDE)),
            dma((2,)),
            dma((4, 10)),
            dma,
            dma,
            dma,
            dma((11,)),
            dma((1,)),
            pltpu.SemaphoreType.REGULAR((2,)),
            pltpu.SemaphoreType.REGULAR,
        ],
        compiler_params=pltpu.CompilerParams(
            collective_id=0, has_side_effects=True, vmem_limit_bytes=55040 * 1024
        ),
        name="merge",
    )(expert_grams, expert_weights)
    return merged, ratio[0, 0]


def solution(mesh):
    placed = (P(None, "row", None), P(None, "row", "grp"))
    return jax.shard_map(
        local, mesh=mesh, in_specs=placed, out_specs=(P("row", "grp"), P()), check_vma=False
    )
```
